32 devices in a mesh: span: 8 (over y, x, core), head: 4 (over z), rep: 1.
Axes of the slice: x: 2, y: 2, z: 4, core: 2. Of those that a mesh axis runs over, the one named last changes fastest.
Arguments:
- queries: bfloat16 [4096, 4096], P(('rep', 'span', 'head')), may hold values from -9 to 9
- keys: bfloat16 [4096, 512], P(('rep', 'span', 'head')), may hold values from -9 to 9
- values: bfloat16 [4096, 512], P(('rep', 'span', 'head')), may hold values from -6 to 6
- out_grad: bfloat16 [4096, 4096], P(('rep', 'span'), 'head'), may hold values from -6 to 6
- doc_lengths: int32 [4], P('rep'), may hold values from 1 to 2048, 4096 in all
Outputs:
- key_value_grads: bfloat16 [1024, 4096], P('head', ('rep', 'span'))
- log_totals: float32 [32, 4096], P('head', ('rep', 'span'))
The draws below stay inside these ranges and needn't reach their ends.
Inputs may be any that keep to these rules, and one draw needn't show every extreme that they name: `doc_lengths`: they sum to 4096; the longest is exactly 2048.
All inputs are finite; a program needn't handle non-finite values.
Results may differ from the reference program's by a relative error of at most 0.0068.
Values may be sent and summed in bfloat16 or wider, within the bound.
A program may use at most 64 MiB of HBM per device.

```python
import math
import jax
import jax.numpy as jnp
import numpy as np
from jax import lax

HEADS = 32
KV_HEADS = 4
HEAD_DIM = 128
BLOCK = 128
WINDOW = 2
TOKENS = 4096
HALO = 128
MOST_DOC = 2048
DOCS = 4


def draw_queries(key, part):
    fresh_key = jax.random.fold_in(key, 11)
    drawn = jax.random.truncated_normal(fresh_key, -6.0, 6.0, (TOKENS, HEADS * HEAD_DIM), jnp.float32)
    return drawn.astype(jnp.bfloat16)


def draw_keys(key, part):
    fresh_key = jax.random.fold_in(key, 13)
    drawn = jax.random.truncated_normal(fresh_key, -6.0, 6.0, (TOKENS, KV_HEADS * HEAD_DIM), jnp.float32)
    return drawn.astype(jnp.bfloat16)


def block_levels(rng, extent, pieces, least, high):
    loudness, own = 1.0, jax.random.fold_in(rng, 6)
    for position, parts in pieces:
        steps = jnp.exp(jax.random.uniform(jax.random.fold_in(own, position), (parts,), jnp.float32, least / len(pieces), high / len(pieces)))
        loudness = loudness * jnp.repeat(steps, extent[position] // parts).reshape([-1 if axis == position else 1 for axis in range(len(extent))])
    return loudness


def profile(number_of, total, most, lean):
    weights = [(1 << 20) // math.isqrt(rank ** lean) + 1 for rank in range(2, number_of + 1)]
    rest, holding = total - most - (number_of - 1), [1] * (number_of - 1)
    while rest > 0:
        movable = [i for i in range(number_of - 1) if holding[i] < most]
        pool, remaining = sum([weights[i] for i in movable]), rest
        for i in movable:
            more = min(most - holding[i], max(1, remaining * weights[i] // pool), rest)
            holding[i] = holding[i] + more
            rest = rest - more
    return np.array([most] + holding)


def ragged_sizes(own_key, number_of, total, bound, lean):
    if number_of == 2:
        one = jax.random.randint(own_key, (), max(1, total - bound), min(bound, total - 1) + 1)
        return jnp.stack([one, total - one])
    lengths = jnp.asarray(profile(number_of, total, bound, lean), jnp.int32)
    couples = (number_of - 1) // 2
    source_of, sink = lengths[1:1 + 2 * couples:2], lengths[2:2 + 2 * couples:2]
    margin = jnp.minimum(source_of - 1, bound - sink)
    moved = jax.random.randint(jax.random.fold_in(own_key, 1), (couples,), 0, 1 << 20) % (margin + 1)
    lengths = lengths.at[1:1 + 2 * couples:2].set(source_of - moved).at[2:2 + 2 * couples:2].set(sink + moved)
    return lengths[jax.random.permutation(jax.random.fold_in(own_key, 2), number_of)]


def gaussian(own_key, extent, scale, most, cuts=(), kind=jnp.bfloat16):
    entries = jax.random.normal(own_key, extent, jnp.float32) * scale
    if len(cuts) > 0:
        entries = block_levels(own_key, extent, cuts, -0.22, 0.18) * entries
    return jnp.clip(entries, min=-most, max=most).astype(kind)


def setup_inputs(seed: int = 0, part: int = 0) -> dict:
    arg_keys = jax.random.split(jax.random.key(seed), 6)
    part_splits = jax.random.split(jax.random.fold_in(arg_keys[5], part), 6)
    queries = draw_queries(jax.random.fold_in(jax.random.fold_in(arg_keys[5], part), 71), part)
    keys = draw_keys(jax.random.fold_in(jax.random.fold_in(arg_keys[5], part), 71), part)
    values = gaussian(part_splits[2], (TOKENS, KV_HEADS * HEAD_DIM), 1.0, 6.0, ((0, 32),))
    out_grad = gaussian(part_splits[3], (TOKENS, HEADS * HEAD_DIM), 1.0, 6.0, ((0, 8), (1, 4)))
    doc_lengths = ragged_sizes(part_splits[4], DOCS, TOKENS, MOST_DOC, 2).astype(jnp.int32)
    return dict(queries=queries, keys=keys, values=values, out_grad=out_grad, doc_lengths=doc_lengths)


def document_starts(doc_lengths, positions):
    doc_starts = (jnp.cumsum(doc_lengths) - doc_lengths).astype(jnp.int32)
    inside = doc_starts[None, :] <= positions[:, None]
    return lax.optimization_barrier(jnp.max(jnp.where(inside, doc_starts[None, :], 0), axis=1)).astype(jnp.int32)

def reference(queries, keys, values, out_grad, doc_lengths):
    score_scale = 1.0 / math.sqrt(HEAD_DIM)
    group_size = HEADS // KV_HEADS
    width = WINDOW * BLOCK
    n_blocks = TOKENS // BLOCK
    query_heads = queries.reshape(TOKENS, KV_HEADS, group_size, HEAD_DIM)
    grad_heads = out_grad.reshape(TOKENS, KV_HEADS, group_size, HEAD_DIM)
    padding = jnp.zeros((HALO, KV_HEADS, HEAD_DIM), jnp.bfloat16)
    key_pad = jnp.concatenate([padding, keys.reshape(TOKENS, KV_HEADS, HEAD_DIM)], 0)
    value_pad = jnp.concatenate([padding, values.reshape(TOKENS, KV_HEADS, HEAD_DIM)], 0)
    block_offsets = jnp.arange(BLOCK, dtype=jnp.int32)
    window_offsets = jnp.arange(width, dtype=jnp.int32)

    def block_step(carry, block_index):
        key_grad, value_grad = carry
        first_row = block_index * BLOCK
        query_block = lax.dynamic_slice_in_dim(query_heads, first_row, BLOCK, 0).astype(jnp.float32)
        grad_block = lax.dynamic_slice_in_dim(grad_heads, first_row, BLOCK, 0).astype(jnp.float32)
        key_window = lax.dynamic_slice_in_dim(key_pad, first_row, width, 0).astype(jnp.float32)
        value_window = lax.dynamic_slice_in_dim(value_pad, first_row, width, 0).astype(jnp.float32)
        query_pos = first_row + block_offsets
        key_pos = first_row - HALO + window_offsets
        doc_first = document_starts(doc_lengths, query_pos)
        allowed = (key_pos[None, :] >= doc_first[:, None]) & (key_pos[None, :] <= query_pos[:, None])
        scores = jnp.einsum('qkgd,jkd->kgqj', query_block, key_window) * score_scale
        scores = jnp.where(allowed[None, None], scores, -1e+30)
        row_max = lax.optimization_barrier(jnp.max(scores, axis=-1, keepdims=True))
        exponent = jnp.exp(scores - row_max)
        row_total = lax.optimization_barrier(jnp.sum(exponent, axis=-1, keepdims=True))
        weights = exponent / row_total
        log_totals = (row_max + jnp.log(row_total))[..., 0]
        weights_low = lax.optimization_barrier(weights.astype(jnp.bfloat16)).astype(jnp.float32)
        attention = jnp.einsum('kgqj,jkd->qkgd', weights_low, value_window).astype(jnp.bfloat16)
        attention = lax.optimization_barrier(attention).astype(jnp.float32)
        dweights = jnp.einsum('qkgd,jkd->kgqj', grad_block, value_window)
        delta_rows = jnp.einsum('qkgd,qkgd->kgq', grad_block, attention)
        dscores = (weights * (dweights - delta_rows[..., None])).astype(jnp.bfloat16)
        dscores = lax.optimization_barrier(dscores).astype(jnp.float32)
        key_part = jnp.einsum('kgqj,qkgd->jkd', dscores, query_block) * score_scale
        value_part = jnp.einsum('kgqj,qkgd->jkd', weights_low, grad_block)
        key_grad = lax.dynamic_update_slice_in_dim(key_grad, lax.dynamic_slice_in_dim(key_grad, first_row, width, 0) + key_part, first_row, 0)
        value_grad = lax.dynamic_update_slice_in_dim(value_grad, lax.dynamic_slice_in_dim(value_grad, first_row, width, 0) + value_part, first_row, 0)
        return ((key_grad, value_grad), log_totals.reshape(HEADS, BLOCK))
    zeros_init = jnp.zeros((TOKENS + HALO, KV_HEADS, HEAD_DIM), jnp.float32)
    (key_grad, value_grad), total_blocks = lax.scan(block_step, (zeros_init, zeros_init), jnp.arange(n_blocks, dtype=jnp.int32))
    log_totals = jnp.transpose(total_blocks, (1, 0, 2)).reshape(HEADS, TOKENS)
    stacked = jnp.stack([key_grad[HALO:], value_grad[HALO:]], axis=2)
    key_value_grads = jnp.transpose(stacked, (1, 2, 3, 0)).reshape(2 * KV_HEADS * HEAD_DIM, TOKENS)
    return (key_value_grads.astype(jnp.bfloat16), log_totals)
```

```python
import math

import jax
import jax.numpy as jnp
from jax import lax
from jax.experimental import pallas as pl
from jax.experimental.pallas import tpu as pltpu
from jax.sharding import PartitionSpec as P

HEADS = 32
KV_HEADS = 4
HEAD_DIM = 128
BLOCK = 128
WINDOW = 2
HALO = 128
LOG2E = math.log2(math.e)
LN2 = math.log(2.0)
MESH = pl.DeviceIdType.MESH


def from_partner(block, axis, bit):
    count = lax.axis_size(axis)
    route = []
    for low in range(count):
        high = low | 1 << bit
        if high != low and high < count:
            route += [(low, high), (high, low)]
    return lax.ppermute(block, axis, route)


def passed_along(block, axis, distance):
    devices = range(lax.axis_size(axis))
    route = [(i - distance, i) for i in devices if i - distance in devices]
    return lax.ppermute(block, axis, route)


def group_total(partial_value, sharers, head_index):
    levels = sharers.bit_length() - 1
    for level in reversed(range(levels)):
        half_rows = partial_value.shape[0] // 2
        lower_half = head_index >> level & 1 == 0
        kept_rows = jnp.where(lower_half, partial_value[:half_rows], partial_value[half_rows:])
        given_rows = jnp.where(lower_half, partial_value[half_rows:], partial_value[:half_rows])
        partial_value = kept_rows + from_partner(given_rows, "head", level)
    return partial_value


def shards(queries, keys, values, out_grad, doc_lengths):
    head_count = lax.axis_size("head")
    head_index = lax.axis_index("head")
    span_index = lax.axis_index("span")
    tok_rows = queries.shape[0]
    heads_here = HEADS // head_count
    sharers = head_count // KV_HEADS
    span_len = tok_rows * head_count
    score_scale = 1.0 / math.sqrt(HEAD_DIM)
    query_send = queries.reshape(tok_rows, head_count, heads_here * HEAD_DIM)
    keyval = jnp.concatenate(
        [keys.reshape(tok_rows, KV_HEADS, HEAD_DIM), values.reshape(tok_rows, KV_HEADS, HEAD_DIM)],
        axis=2,
    )
    repeated = jnp.repeat(keyval, sharers, axis=1)
    query_local, pairs_local = (
        lax.all_to_all(query_send, "head", split_axis=1, concat_axis=0, tiled=True),
        lax.all_to_all(repeated, "head", split_axis=1, concat_axis=0, tiled=True),
    )
    pairs_local = pairs_local.reshape(span_len, 2 * HEAD_DIM)
    query_local = query_local.reshape(span_len, heads_here, HEAD_DIM)
    grad_local = out_grad.reshape(span_len, heads_here, HEAD_DIM)
    earlier = passed_along(pairs_local[span_len - HALO :], "span", 1)
    extended = jnp.concatenate([earlier, pairs_local], 0)
    base_row = span_index * span_len
    doc_starts = jnp.cumsum(doc_lengths) - doc_lengths
    query_pos = base_row + jnp.arange(span_len, dtype=jnp.int32)
    doc_first = jnp.max(
        jnp.where(doc_starts[None, :] <= query_pos[:, None], doc_starts[None, :], 0), axis=1
    )
    n_blocks = span_len // BLOCK
    per_group = min(n_blocks, max(1, 512 // BLOCK))
    n_groups = n_blocks // per_group
    group_rows = per_group * BLOCK
    width = WINDOW * BLOCK
    block_offsets = jnp.arange(BLOCK, dtype=jnp.int32)
    window_offsets = jnp.arange(width, dtype=jnp.int32)
    block_starts = jnp.arange(per_group, dtype=jnp.int32) * BLOCK

    def attend(gradients, group_index):
        first_row = group_index * group_rows
        query_group = lax.dynamic_slice_in_dim(query_local, first_row, group_rows, 0).reshape(
            per_group, BLOCK, heads_here, HEAD_DIM
        )
        grad_group = lax.dynamic_slice_in_dim(grad_local, first_row, group_rows, 0).reshape(
            per_group, BLOCK, heads_here, HEAD_DIM
        )
        pair_rows = lax.dynamic_slice_in_dim(extended, first_row, group_rows + HALO, 0).reshape(
            per_group + WINDOW - 1, BLOCK, 2 * HEAD_DIM
        )
        window = jnp.stack(
            [pair_rows[shift_index : shift_index + per_group] for shift_index in range(WINDOW)],
            axis=1,
        ).reshape(per_group, width, 2 * HEAD_DIM)
        key_window = window[..., :HEAD_DIM]
        value_window = window[..., HEAD_DIM:]
        query_rows = base_row + first_row + block_starts[:, None] + block_offsets[None, :]
        key_rows = base_row + first_row - HALO + block_starts[:, None] + window_offsets[None, :]
        first_doc = lax.dynamic_slice_in_dim(doc_first, first_row, group_rows, 0).reshape(
            per_group, BLOCK
        )
        allowed = (key_rows[:, None, :] >= first_doc[:, :, None]) & (
            key_rows[:, None, :] <= query_rows[:, :, None]
        )
        scores = (
            jnp.einsum(
                "gqhd,gkd->ghqk", query_group, key_window, preferred_element_type=jnp.float32
            )
            * score_scale
        )
        scores = jnp.where(allowed[:, None], scores, -1e30)
        row_max = jnp.max(scores, axis=-1, keepdims=True)
        exponent = jnp.exp(scores - row_max)
        row_total = jnp.sum(exponent, axis=-1, keepdims=True)
        weights = exponent / row_total
        log_totals = (row_max + jnp.log(row_total))[..., 0]
        weights_low = weights.astype(jnp.bfloat16)
        attention = jnp.einsum(
            "ghqk,gkd->gqhd", weights_low, value_window, preferred_element_type=jnp.float32
        ).astype(jnp.bfloat16)
        attention = lax.optimization_barrier(attention).astype(jnp.float32)
        dweights = jnp.einsum(
            "gqhd,gkd->ghqk", grad_group, value_window, preferred_element_type=jnp.float32
        )
        delta_rows = jnp.einsum("gqhd,gqhd->ghq", grad_group.astype(jnp.float32), attention)
        dscores = (weights * (dweights - delta_rows[..., None])).astype(jnp.bfloat16)
        key_part = (
            jnp.einsum("ghqk,gqhd->gkd", dscores, query_group, preferred_element_type=jnp.float32)
            * score_scale
        )
        value_part = jnp.einsum(
            "ghqk,gqhd->gkd", weights_low, grad_group, preferred_element_type=jnp.float32
        )
        pieces = jnp.concatenate([key_part, value_part], -1).reshape(
            per_group, WINDOW, BLOCK, 2 * HEAD_DIM
        )
        folded = jnp.zeros((per_group + WINDOW - 1, BLOCK, 2 * HEAD_DIM), jnp.float32)
        for shift_index in range(WINDOW):
            folded = folded.at[shift_index : shift_index + per_group].add(pieces[:, shift_index])
        folded = folded.reshape(group_rows + HALO, 2 * HEAD_DIM)
        current = lax.dynamic_slice_in_dim(gradients, first_row, group_rows + HALO, 0)
        gradients = lax.dynamic_update_slice_in_dim(gradients, current + folded, first_row, 0)
        return (gradients, jnp.transpose(log_totals, (1, 0, 2)).reshape(heads_here, group_rows))

    gradients, total_groups = lax.scan(
        attend,
        jnp.zeros((HALO + span_len, 2 * HEAD_DIM), jnp.float32),
        jnp.arange(n_groups, dtype=jnp.int32),
    )
    log_totals = jnp.transpose(total_groups, (1, 0, 2)).reshape(heads_here, span_len)
    summed = group_total(gradients.T, sharers, head_index)
    returned = passed_along(summed[:, :HALO].astype(jnp.bfloat16), "span", -1).astype(jnp.float32)
    local_grads = summed[:, HALO:].at[:, span_len - HALO :].add(returned)
    return (local_grads.astype(jnp.bfloat16), log_totals)


def attend_kernel(
    lengths_hbm, queries, keys, values, out_grad,
    grads_out, totals_out,
    lengths, query_buf, key_buf, value_buf, query_slots, key_ext, value_ext, grad_buf,
    bias, key_acc, value_acc, halo_send, halo_recv, total_rows,
    local_sems, pair_send, pair_recv, query_send, query_recv, edge_send, edge_recv,
    ready, span_ready,
):
    span = lax.axis_index("span")
    spans = lax.axis_size("span")
    me = lax.axis_index("head")
    peers = lax.axis_size("head")
    last = peers - 1
    rows = queries.shape[0]
    head_cols = queries.shape[1] // peers
    piece_cols = 2 * HEAD_DIM
    pieces = head_cols // piece_cols
    width = WINDOW * BLOCK
    final = peers // 2 - me // (peers // 2)
    second = 1 - jnp.minimum(me, 1)
    order = (me, second, 6 - me - second - final, final)

    def column(index, size):
        return pl.ds(pl.multiple_of(index * size, size), size)

    own_rows = pl.ds(pl.multiple_of(HALO + me * rows, rows), rows)
    loads = [
        pltpu.make_async_copy(keys, key_buf, local_sems.at[0]),
        pltpu.make_async_copy(values, value_buf, local_sems.at[1]),
        pltpu.make_async_copy(queries, query_buf, local_sems.at[2]),
        pltpu.make_async_copy(
            keys.at[:, column(me, HEAD_DIM)], key_ext.at[own_rows], local_sems.at[3]
        ),
        pltpu.make_async_copy(
            values.at[:, column(me, HEAD_DIM)], value_ext.at[own_rows], local_sems.at[4]
        ),
        pltpu.make_async_copy(
            queries.at[:, column(me, head_cols)], query_slots.at[me], local_sems.at[5]
        ),
        pltpu.make_async_copy(out_grad, grad_buf, local_sems.at[6]),
        pltpu.make_async_copy(lengths_hbm, lengths, local_sems.at[7]),
    ]
    for load in loads:
        load.start()

    barrier = pltpu.get_barrier_semaphore()
    for peer in range(1, peers):

        @pl.when(peer > me)
        def _():
            pl.semaphore_signal(barrier, inc=1, device_id={"head": peer}, device_id_type=MESH)

    @pl.when(span < spans - 1)
    def _():
        pl.semaphore_signal(barrier, inc=1, device_id={"span": span + 1}, device_id_type=MESH)

    @pl.when(me + span > 0)
    def _():
        pl.semaphore_wait(barrier, me + jnp.minimum(span, 1))

    for peer in range(peers - 1):

        @pl.when(peer < me)
        def _():
            pl.semaphore_signal(
                ready.at[me], inc=1, device_id={"head": peer}, device_id_type=MESH
            )

    @pl.when(span > 0)
    def _():
        pl.semaphore_signal(span_ready, inc=1, device_id={"span": span - 1}, device_id_type=MESH)

    def pair_copy(which, buf, ext, source, target):
        return pltpu.make_async_remote_copy(
            src_ref=buf.at[:, column(target, HEAD_DIM)],
            dst_ref=ext.at[pl.ds(pl.multiple_of(HALO + source * rows, rows), rows)],
            send_sem=pair_send.at[which, target],
            recv_sem=pair_recv.at[which, source],
            device_id={"head": target},
            device_id_type=MESH,
        )

    def query_copy(piece, source, target):
        return pltpu.make_async_remote_copy(
            src_ref=query_buf.at[:, column(target * pieces + piece, piece_cols)],
            dst_ref=query_slots.at[source, :, column(piece, piece_cols)],
            send_sem=query_send.at[target, piece],
            recv_sem=query_recv.at[source, piece],
            device_id={"head": target},
            device_id_type=MESH,
        )

    def send_pairs(peer):
        pair_copy(0, key_buf, key_ext, me, peer).start()
        pair_copy(1, value_buf, value_ext, me, peer).start()

    def send_queries(peer):
        for piece in range(pieces):
            query_copy(piece, me, peer).start()

    loads[0].wait()
    loads[1].wait()
    for peer in range(peers - 1):

        @pl.when(peer < me)
        def _():
            send_pairs(peer)

    loads[2].wait()
    for peer in range(peers - 1):

        @pl.when(peer < me)
        def _():
            send_queries(peer)

    for peer in range(1, peers):

        @pl.when(peer > me)
        def _():
            pl.semaphore_wait(ready.at[peer], 1)
            send_pairs(peer)

    for peer in reversed(range(1, peers)):

        @pl.when(peer > me)
        def _():
            send_queries(peer)

    key_acc[...] = jnp.zeros_like(key_acc)
    value_acc[...] = jnp.zeros_like(value_acc)
    for load in loads[3:]:
        load.wait()

    def wait_pairs(peer):
        @pl.when(peer != me)
        def _():
            pair_copy(0, key_buf, key_ext, peer, me).wait_recv()
            pair_copy(1, value_buf, value_ext, peer, me).wait_recv()

    def halo_copy(which, ext):
        return pltpu.make_async_remote_copy(
            src_ref=ext.at[pl.ds(peers * rows, HALO)],
            dst_ref=ext.at[pl.ds(0, HALO)],
            send_sem=edge_send.at[which],
            recv_sem=edge_recv.at[which],
            device_id={"span": span + 1},
            device_id_type=MESH,
        )

    return_copy = pltpu.make_async_remote_copy(
        src_ref=halo_send,
        dst_ref=halo_recv,
        send_sem=edge_send.at[2],
        recv_sem=edge_recv.at[2],
        device_id={"span": span - 1},
        device_id_type=MESH,
    )

    wait_pairs(last)

    @pl.when(span < spans - 1)
    def _():
        pl.semaphore_wait(span_ready, 1)
        halo_copy(0, key_ext).start()
        halo_copy(1, value_ext).start()

    for peer in range(last):
        wait_pairs(peer)

    @pl.when(span > 0)
    def _():
        halo_copy(0, key_ext).wait_recv()
        halo_copy(1, value_ext).wait_recv()

    @pl.when(span == 0)
    def _():
        key_ext[pl.ds(0, HALO)] = jnp.zeros((HALO, HEAD_DIM), jnp.bfloat16)
        value_ext[pl.ds(0, HALO)] = jnp.zeros((HALO, HEAD_DIM), jnp.bfloat16)

    score_scale = 1.0 / math.sqrt(HEAD_DIM)
    contract_last = (((1,), (1,)), ((), ()))

    def stacked(block):
        return jnp.concatenate([block[:, :HEAD_DIM], block[:, HEAD_DIM:]], axis=0)

    def write(done):
        held = pl.ds(HALO + done * BLOCK, BLOCK)
        cols = pl.ds(done * BLOCK, BLOCK)
        key_part = key_acc[held] * score_scale
        grads_out[pl.ds(0, HEAD_DIM), cols] = key_part.T.astype(jnp.bfloat16)
        grads_out[pl.ds(HEAD_DIM, HEAD_DIM), cols] = value_acc[held].T.astype(jnp.bfloat16)

    def put_totals(block):
        for head in range(2 * pieces):
            totals_out[head : head + 1, block * BLOCK : (block + 1) * BLOCK] = total_rows[
                block * pieces + head // 2, head % 2 : head % 2 + 1
            ]

    for step in range(4):
        block = order[step]
        first_row = pl.multiple_of(block * BLOCK, BLOCK)
        window = pl.ds(first_row, width)
        base = (span * peers + block) * BLOCK
        query_pos = base + lax.broadcasted_iota(jnp.int32, (1, BLOCK), 1)
        first = jnp.zeros((1, BLOCK), jnp.int32)
        start = jnp.int32(0)
        for doc in range(lengths.shape[0]):
            first = jnp.maximum(first, jnp.where(query_pos >= start, start, 0))
            start = start + lengths[doc]
        key_pos = base - HALO + lax.broadcasted_iota(jnp.int32, (width, BLOCK), 0)
        allowed = (key_pos >= first) & (key_pos <= query_pos)
        bias[...] = jnp.where(allowed, 0.0, -1e30)

        def one_piece(piece, carry, block=block, first_row=first_row, window=window, step=step):
            if step > 0:
                query_copy(piece, block, me).wait_recv()
            cols = column(piece, piece_cols)
            query_pair = stacked(query_slots[block, :, cols])
            grad_pair = stacked(grad_buf[pl.ds(first_row, BLOCK), cols])
            scores = lax.dot_general(
                key_ext[window], query_pair, contract_last, preferred_element_type=jnp.float32
            )
            dweights = lax.dot_general(
                value_ext[window], grad_pair, contract_last, preferred_element_type=jnp.float32
            )
            shift = bias[...]
            scores = scores * (score_scale * LOG2E) + jnp.concatenate([shift, shift], axis=1)
            row_max = jnp.max(scores, axis=0, keepdims=True)
            exponent = jnp.exp2(scores - row_max)
            row_total = jnp.sum(exponent, axis=0, keepdims=True)
            weights = exponent * (1.0 / row_total)
            weights_low = weights.astype(jnp.bfloat16)
            delta = jnp.sum(weights * dweights, axis=0, keepdims=True)
            dscores = (weights * (dweights - delta)).astype(jnp.bfloat16)
            key_acc[window] += jnp.dot(dscores, query_pair, preferred_element_type=jnp.float32)
            value_acc[window] += jnp.dot(weights_low, grad_pair, preferred_element_type=jnp.float32)
            totals = row_max * LN2 + jnp.log(row_total)
            for half in range(2):
                total_rows[block * pieces + piece, half : half + 1] = totals[
                    :, half * BLOCK : (half + 1) * BLOCK
                ]
            return carry

        if step == 3:
            for done in range(peers - 1):

                @pl.when((done != block) & (done != block - 1))
                def _():
                    write(done)

            @pl.when(span < spans - 1)
            def _():
                return_copy.wait_recv()
                held = pl.ds(last * BLOCK + HALO, BLOCK)
                returned = halo_recv[...].astype(jnp.float32)
                key_acc[held] += returned[:HALO]
                value_acc[held] += returned[HALO:]

            write(last)
            for done in range(peers):

                @pl.when(done != block)
                def _():
                    put_totals(done)

        lax.fori_loop(0, pieces, one_piece, 0)

        @pl.when((block == 0) & (span > 0))
        def _():
            halo_send[pl.ds(0, HALO)] = key_acc[pl.ds(0, HALO)].astype(jnp.bfloat16)
            halo_send[pl.ds(HALO, HALO)] = value_acc[pl.ds(0, HALO)].astype(jnp.bfloat16)
            return_copy.start()

    for done in range(1, peers - 1):

        @pl.when(done == final)
        def _():
            write(done - 1)
            write(done)
            put_totals(done)

    for peer in order[1:]:
        pair_copy(0, key_buf, key_ext, me, peer).wait_send()
        pair_copy(1, value_buf, value_ext, me, peer).wait_send()
        for piece in range(pieces):
            query_copy(piece, me, peer).wait_send()

    @pl.when(span < spans - 1)
    def _():
        halo_copy(0, key_ext).wait_send()
        halo_copy(1, value_ext).wait_send()

    @pl.when(span > 0)
    def _():
        return_copy.wait_send()


def put_out(grads, totals, grads_out, totals_out, sems):
    copies = [
        pltpu.make_async_copy(grads, grads_out, sems.at[0]),
        pltpu.make_async_copy(totals, totals_out, sems.at[1]),
    ]
    for copy in copies:
        copy.start()
    for copy in copies:
        copy.wait()


def fused_shards(queries, keys, values, out_grad, doc_lengths):
    head_count = lax.axis_size("head")
    rows = queries.shape[0]
    span_len = rows * head_count
    head_cols = queries.shape[1] // head_count
    heads_here = HEADS // head_count
    pieces = heads_here // 2
    any_space = pl.BlockSpec(memory_space=pl.ANY)
    vmem = pl.BlockSpec(memory_space=pltpu.VMEM)
    dma = pltpu.SemaphoreType.DMA
    held = pl.pallas_call(
        attend_kernel,
        out_shape=(
            pltpu.VMEM((2 * HEAD_DIM, span_len), jnp.bfloat16),
            pltpu.VMEM((heads_here, span_len), jnp.float32),
        ),
        in_specs=[any_space] * 5,
        out_specs=(vmem, vmem),
        scratch_shapes=[
            pltpu.SMEM(doc_lengths.shape, jnp.int32),
            pltpu.VMEM(queries.shape, jnp.bfloat16),
            pltpu.VMEM(keys.shape, jnp.bfloat16),
            pltpu.VMEM(values.shape, jnp.bfloat16),
            pltpu.VMEM((head_count, rows, head_cols), jnp.bfloat16),
            pltpu.VMEM((HALO + span_len, HEAD_DIM), jnp.bfloat16),
            pltpu.VMEM((HALO + span_len, HEAD_DIM), jnp.bfloat16),
            pltpu.VMEM(out_grad.shape, jnp.bfloat16),
            pltpu.VMEM((WINDOW * BLOCK, BLOCK), jnp.float32),
            pltpu.VMEM((HALO + span_len, HEAD_DIM), jnp.float32),
            pltpu.VMEM((HALO + span_len, HEAD_DIM), jnp.float32),
            pltpu.VMEM((2 * HALO, HEAD_DIM), jnp.bfloat16),
            pltpu.VMEM((2 * HALO, HEAD_DIM), jnp.bfloat16),
            pltpu.VMEM((head_count * pieces, 8, BLOCK), jnp.float32),
            dma((8,)),
            dma((2, head_count)),
            dma((2, head_count)),
            dma((head_count, pieces)),
            dma((head_count, pieces)),
            dma((3,)),
            dma((3,)),
            pltpu.SemaphoreType.REGULAR((head_count,)),
            pltpu.SemaphoreType.REGULAR,
        ],
        compiler_params=pltpu.CompilerParams(collective_id=0, has_side_effects=True),
        name="attend",
    )(doc_lengths, queries, keys, values, out_grad)
    return pl.pallas_call(
        put_out,
        out_shape=tuple(jax.ShapeDtypeStruct(one.shape, one.dtype) for one in held),
        in_specs=[vmem, vmem],
        out_specs=(any_space, any_space),
        scratch_shapes=[dma((2,))],
        name="put_out",
    )(*[pltpu.with_memory_space_constraint(one, pltpu.VMEM) for one in held])


def pick_shards(queries, keys, values, out_grad, doc_lengths):
    head_count = lax.axis_size("head")
    if head_count == KV_HEADS == 4 and queries.shape[0] == BLOCK == HALO:
        return fused_shards(queries, keys, values, out_grad, doc_lengths)
    return shards(queries, keys, values, out_grad, doc_lengths)


def solution(mesh):
    return jax.shard_map(
        pick_shards,
        mesh=mesh,
        in_specs=(
            P(("rep", "span", "head"), None),
            P(("rep", "span", "head"), None),
            P(("rep", "span", "head"), None),
            P(("rep", "span"), "head"),
            P("rep"),
        ),
        out_specs=(P("head", ("rep", "span")), P("head", ("rep", "span"))),
        check_vma=False,
    )
```

```python
import math

import jax
import jax.numpy as jnp
from jax import lax
from jax.experimental import pallas as pl
from jax.experimental.pallas import tpu as pltpu
from jax.sharding import PartitionSpec as P

HEADS = 32
KV_HEADS = 4
HEAD_DIM = 128
BLOCK = 128
WINDOW = 2
HALO = 128
LOG2E = math.log2(math.e)
LN2 = math.log(2.0)
MESH = pl.DeviceIdType.MESH


def from_partner(block, axis, bit):
    count = lax.axis_size(axis)
    route = []
    for low in range(count):
        high = low | 1 << bit
        if high != low and high < count:
            route += [(low, high), (high, low)]
    return lax.ppermute(block, axis, route)


def passed_along(block, axis, distance):
    devices = range(lax.axis_size(axis))
    route = [(i - distance, i) for i in devices if i - distance in devices]
    return lax.ppermute(block, axis, route)


def group_total(partial_value, sharers, head_index):
    levels = sharers.bit_length() - 1
    for level in reversed(range(levels)):
        half_rows = partial_value.shape[0] // 2
        lower_half = head_index >> level & 1 == 0
        kept_rows = jnp.where(lower_half, partial_value[:half_rows], partial_value[half_rows:])
        given_rows = jnp.where(lower_half, partial_value[half_rows:], partial_value[:half_rows])
        partial_value = kept_rows + from_partner(given_rows, "head", level)
    return partial_value


def shards(queries, keys, values, out_grad, doc_lengths):
    head_count = lax.axis_size("head")
    head_index = lax.axis_index("head")
    span_index = lax.axis_index("span")
    tok_rows = queries.shape[0]
    heads_here = HEADS // head_count
    sharers = head_count // KV_HEADS
    span_len = tok_rows * head_count
    score_scale = 1.0 / math.sqrt(HEAD_DIM)
    query_send = queries.reshape(tok_rows, head_count, heads_here * HEAD_DIM)
    keyval = jnp.concatenate(
        [keys.reshape(tok_rows, KV_HEADS, HEAD_DIM), values.reshape(tok_rows, KV_HEADS, HEAD_DIM)],
        axis=2,
    )
    repeated = jnp.repeat(keyval, sharers, axis=1)
    query_local, pairs_local = (
        lax.all_to_all(query_send, "head", split_axis=1, concat_axis=0, tiled=True),
        lax.all_to_all(repeated, "head", split_axis=1, concat_axis=0, tiled=True),
    )
    pairs_local = pairs_local.reshape(span_len, 2 * HEAD_DIM)
    query_local = query_local.reshape(span_len, heads_here, HEAD_DIM)
    grad_local = out_grad.reshape(span_len, heads_here, HEAD_DIM)
    earlier = passed_along(pairs_local[span_len - HALO :], "span", 1)
    extended = jnp.concatenate([earlier, pairs_local], 0)
    base_row = span_index * span_len
    doc_starts = jnp.cumsum(doc_lengths) - doc_lengths
    query_pos = base_row + jnp.arange(span_len, dtype=jnp.int32)
    doc_first = jnp.max(
        jnp.where(doc_starts[None, :] <= query_pos[:, None], doc_starts[None, :], 0), axis=1
    )
    n_blocks = span_len // BLOCK
    per_group = min(n_blocks, max(1, 512 // BLOCK))
    n_groups = n_blocks // per_group
    group_rows = per_group * BLOCK
    width = WINDOW * BLOCK
    block_offsets = jnp.arange(BLOCK, dtype=jnp.int32)
    window_offsets = jnp.arange(width, dtype=jnp.int32)
    block_starts = jnp.arange(per_group, dtype=jnp.int32) * BLOCK

    def attend(gradients, group_index):
        first_row = group_index * group_rows
        query_group = lax.dynamic_slice_in_dim(query_local, first_row, group_rows, 0).reshape(
            per_group, BLOCK, heads_here, HEAD_DIM
        )
        grad_group = lax.dynamic_slice_in_dim(grad_local, first_row, group_rows, 0).reshape(
            per_group, BLOCK, heads_here, HEAD_DIM
        )
        pair_rows = lax.dynamic_slice_in_dim(extended, first_row, group_rows + HALO, 0).reshape(
            per_group + WINDOW - 1, BLOCK, 2 * HEAD_DIM
        )
        window = jnp.stack(
            [pair_rows[shift_index : shift_index + per_group] for shift_index in range(WINDOW)],
            axis=1,
        ).reshape(per_group, width, 2 * HEAD_DIM)
        key_window = window[..., :HEAD_DIM]
        value_window = window[..., HEAD_DIM:]
        query_rows = base_row + first_row + block_starts[:, None] + block_offsets[None, :]
        key_rows = base_row + first_row - HALO + block_starts[:, None] + window_offsets[None, :]
        first_doc = lax.dynamic_slice_in_dim(doc_first, first_row, group_rows, 0).reshape(
            per_group, BLOCK
        )
        allowed = (key_rows[:, None, :] >= first_doc[:, :, None]) & (
            key_rows[:, None, :] <= query_rows[:, :, None]
        )
        scores = (
            jnp.einsum(
                "gqhd,gkd->ghqk", query_group, key_window, preferred_element_type=jnp.float32
            )
            * score_scale
        )
        scores = jnp.where(allowed[:, None], scores, -1e30)
        row_max = jnp.max(scores, axis=-1, keepdims=True)
        exponent = jnp.exp(scores - row_max)
        row_total = jnp.sum(exponent, axis=-1, keepdims=True)
        weights = exponent / row_total
        log_totals = (row_max + jnp.log(row_total))[..., 0]
        weights_low = weights.astype(jnp.bfloat16)
        attention = jnp.einsum(
            "ghqk,gkd->gqhd", weights_low, value_window, preferred_element_type=jnp.float32
        ).astype(jnp.bfloat16)
        attention = lax.optimization_barrier(attention).astype(jnp.float32)
        dweights = jnp.einsum(
            "gqhd,gkd->ghqk", grad_group, value_window, preferred_element_type=jnp.float32
        )
        delta_rows = jnp.einsum("gqhd,gqhd->ghq", grad_group.astype(jnp.float32), attention)
        dscores = (weights * (dweights - delta_rows[..., None])).astype(jnp.bfloat16)
        key_part = (
            jnp.einsum("ghqk,gqhd->gkd", dscores, query_group, preferred_element_type=jnp.float32)
            * score_scale
        )
        value_part = jnp.einsum(
            "ghqk,gqhd->gkd", weights_low, grad_group, preferred_element_type=jnp.float32
        )
        pieces = jnp.concatenate([key_part, value_part], -1).reshape(
            per_group, WINDOW, BLOCK, 2 * HEAD_DIM
        )
        folded = jnp.zeros((per_group + WINDOW - 1, BLOCK, 2 * HEAD_DIM), jnp.float32)
        for shift_index in range(WINDOW):
            folded = folded.at[shift_index : shift_index + per_group].add(pieces[:, shift_index])
        folded = folded.reshape(group_rows + HALO, 2 * HEAD_DIM)
        current = lax.dynamic_slice_in_dim(gradients, first_row, group_rows + HALO, 0)
        gradients = lax.dynamic_update_slice_in_dim(gradients, current + folded, first_row, 0)
        return (gradients, jnp.transpose(log_totals, (1, 0, 2)).reshape(heads_here, group_rows))

    gradients, total_groups = lax.scan(
        attend,
        jnp.zeros((HALO + span_len, 2 * HEAD_DIM), jnp.float32),
        jnp.arange(n_groups, dtype=jnp.int32),
    )
    log_totals = jnp.transpose(total_groups, (1, 0, 2)).reshape(heads_here, span_len)
    summed = group_total(gradients.T, sharers, head_index)
    returned = passed_along(summed[:, :HALO].astype(jnp.bfloat16), "span", -1).astype(jnp.float32)
    local_grads = summed[:, HALO:].at[:, span_len - HALO :].add(returned)
    return (local_grads.astype(jnp.bfloat16), log_totals)


def attend_kernel(
    lengths_hbm, queries, keys, values, out_grad,
    grads_out, totals_out,
    lengths, query_buf, key_buf, value_buf, query_slots, key_ext, value_ext, grad_buf,
    bias, key_acc, value_acc, halo_send, halo_recv, total_rows,
    local_sems, pair_send, pair_recv, query_send, query_recv, edge_send, edge_recv,
    ready, span_ready,
):
    span = lax.axis_index("span")
    spans = lax.axis_size("span")
    me = lax.axis_index("head")
    peers = lax.axis_size("head")
    last = peers - 1
    rows = queries.shape[0]
    head_cols = queries.shape[1] // peers
    piece_cols = 2 * HEAD_DIM
    pieces = head_cols // piece_cols
    width = WINDOW * BLOCK
    def by_place(*choices):
        pick = choices[0]
        for place in range(1, len(choices)):
            pick = jnp.where(me == place, choices[place], pick)
        return pick

    final = by_place(2, 2, 1, 1)
    order = (by_place(0, 1, 2, 0), by_place(3, 0, 0, 3), by_place(1, 3, 3, 2), final)

    def column(index, size):
        return pl.ds(pl.multiple_of(index * size, size), size)

    own_rows = pl.ds(pl.multiple_of(HALO + me * rows, rows), rows)
    loads = [
        pltpu.make_async_copy(keys, key_buf, local_sems.at[0]),
        pltpu.make_async_copy(values, value_buf, local_sems.at[1]),
        pltpu.make_async_copy(queries, query_buf, local_sems.at[2]),
        pltpu.make_async_copy(
            keys.at[:, column(me, HEAD_DIM)], key_ext.at[own_rows], local_sems.at[3]
        ),
        pltpu.make_async_copy(
            values.at[:, column(me, HEAD_DIM)], value_ext.at[own_rows], local_sems.at[4]
        ),
        pltpu.make_async_copy(
            queries.at[:, column(me, head_cols)], query_slots.at[me], local_sems.at[5]
        ),
        pltpu.make_async_copy(out_grad, grad_buf, local_sems.at[6]),
        pltpu.make_async_copy(lengths_hbm, lengths, local_sems.at[7]),
    ]
    for load in loads[:3]:
        load.start()

    barrier = pltpu.get_barrier_semaphore()
    for peer in range(1, peers):

        @pl.when(peer > me)
        def _():
            pl.semaphore_signal(barrier, inc=1, device_id={"head": peer}, device_id_type=MESH)

    @pl.when(span < spans - 1)
    def _():
        pl.semaphore_signal(barrier, inc=1, device_id={"span": span + 1}, device_id_type=MESH)

    @pl.when(me + span > 0)
    def _():
        pl.semaphore_wait(barrier, me + jnp.minimum(span, 1))

    for peer in range(peers - 1):

        @pl.when(peer < me)
        def _():
            pl.semaphore_signal(
                ready.at[me], inc=1, device_id={"head": peer}, device_id_type=MESH
            )

    @pl.when(span > 0)
    def _():
        pl.semaphore_signal(span_ready, inc=1, device_id={"span": span - 1}, device_id_type=MESH)

    def pair_copy(which, buf, ext, source, target):
        return pltpu.make_async_remote_copy(
            src_ref=buf.at[:, column(target, HEAD_DIM)],
            dst_ref=ext.at[pl.ds(pl.multiple_of(HALO + source * rows, rows), rows)],
            send_sem=pair_send.at[which, target],
            recv_sem=pair_recv.at[which, source],
            device_id={"head": target},
            device_id_type=MESH,
        )

    def query_copy(piece, source, target):
        return pltpu.make_async_remote_copy(
            src_ref=query_buf.at[:, column(target * pieces + piece, piece_cols)],
            dst_ref=query_slots.at[source, :, column(piece, piece_cols)],
            send_sem=query_send.at[target, piece],
            recv_sem=query_recv.at[source, piece],
            device_id={"head": target},
            device_id_type=MESH,
        )

    def send_pairs(peer):
        pair_copy(0, key_buf, key_ext, me, peer).start()
        pair_copy(1, value_buf, value_ext, me, peer).start()

    def send_queries(peer, some=range(pieces)):
        for piece in some:
            query_copy(piece, me, peer).start()

    loads[0].wait()
    loads[1].wait()
    for peer in range(peers - 1):

        @pl.when(peer < me)
        def _():
            send_pairs(peer)

    loads[2].wait()
    for peer in range(peers - 1):

        @pl.when(peer < me)
        def _():
            send_queries(peer)

    for peer in range(1, peers):

        @pl.when(peer > me)
        def _():
            pl.semaphore_wait(ready.at[peer], 1)
            send_pairs(peer)

        if peer == peers // 2:

            @pl.when(peer == me + 1)
            def _():
                send_queries(peer, range(1))

    @pl.when(me == 0)
    def _():
        send_queries(1)

    for peer in reversed(range(2, peers)):

        @pl.when(peer > me)
        def _():
            if peer == peers // 2:

                @pl.when(peer > me + 1)
                def _():
                    send_queries(peer, range(1))

                send_queries(peer, range(1, pieces))
            else:
                send_queries(peer)

    for load in loads[3:]:
        load.start()

    key_acc[...] = jnp.zeros_like(key_acc)
    value_acc[...] = jnp.zeros_like(value_acc)
    for load in loads[3:]:
        load.wait()

    def wait_pairs(peer, wanted=True):
        @pl.when((peer != me) & wanted)
        def _():
            pair_copy(0, key_buf, key_ext, peer, me).wait_recv()
            pair_copy(1, value_buf, value_ext, peer, me).wait_recv()

    def halo_copy(which, ext):
        return pltpu.make_async_remote_copy(
            src_ref=ext.at[pl.ds(peers * rows, HALO)],
            dst_ref=ext.at[pl.ds(0, HALO)],
            send_sem=edge_send.at[which],
            recv_sem=edge_recv.at[which],
            device_id={"span": span + 1},
            device_id_type=MESH,
        )

    return_copy = pltpu.make_async_remote_copy(
        src_ref=halo_send,
        dst_ref=halo_recv,
        send_sem=edge_send.at[2],
        recv_sem=edge_recv.at[2],
        device_id={"span": span - 1},
        device_id_type=MESH,
    )

    wait_pairs(last)

    @pl.when(span < spans - 1)
    def _():
        pl.semaphore_wait(span_ready, 1)
        halo_copy(0, key_ext).start()
        halo_copy(1, value_ext).start()


    score_scale = 1.0 / math.sqrt(HEAD_DIM)
    contract_last = (((1,), (1,)), ((), ()))

    def stacked(block):
        return jnp.concatenate([block[:, :HEAD_DIM], block[:, HEAD_DIM:]], axis=0)

    def write(done):
        held = pl.ds(HALO + done * BLOCK, BLOCK)
        cols = pl.ds(done * BLOCK, BLOCK)
        key_part = key_acc[held] * score_scale
        grads_out[pl.ds(0, HEAD_DIM), cols] = key_part.astype(jnp.bfloat16).T
        grads_out[pl.ds(HEAD_DIM, HEAD_DIM), cols] = value_acc[held].astype(jnp.bfloat16).T

    def put_totals(block):
        for head in range(2 * pieces):
            totals_out[head : head + 1, block * BLOCK : (block + 1) * BLOCK] = total_rows[
                block * pieces + head // 2, head % 2 : head % 2 + 1
            ]

    for step in range(4):
        block = order[step]
        for peer in range(last):
            known = False
            for before in order[:step]:
                known |= (before == peer) | (before == peer + 1)
            wait_pairs(peer, ((block == peer) | (block == peer + 1)) & jnp.logical_not(known))

        @pl.when((block == 0) & (span > 0))
        def _():
            halo_copy(0, key_ext).wait_recv()
            halo_copy(1, value_ext).wait_recv()

        @pl.when((block == 0) & (span == 0))
        def _():
            key_ext[pl.ds(0, HALO)] = jnp.zeros((HALO, HEAD_DIM), jnp.bfloat16)
            value_ext[pl.ds(0, HALO)] = jnp.zeros((HALO, HEAD_DIM), jnp.bfloat16)

        first_row = pl.multiple_of(block * BLOCK, BLOCK)
        window = pl.ds(first_row, width)
        base = (span * peers + block) * BLOCK
        query_pos = base + lax.broadcasted_iota(jnp.int32, (1, BLOCK), 1)
        first = jnp.zeros((1, BLOCK), jnp.int32)
        start = jnp.int32(0)
        for doc in range(lengths.shape[0]):
            first = jnp.maximum(first, jnp.where(query_pos >= start, start, 0))
            start = start + lengths[doc]
        key_pos = base - HALO + lax.broadcasted_iota(jnp.int32, (width, BLOCK), 0)
        allowed = (key_pos >= first) & (key_pos <= query_pos)
        bias[...] = jnp.where(allowed, 0.0, -1e30)

        def one_piece(piece, carry, block=block, first_row=first_row, window=window, step=step):
            @pl.when(block != me)
            def _():
                query_copy(piece, block, me).wait_recv()

            cols = column(piece, piece_cols)
            query_pair = stacked(query_slots[block, :, cols])
            grad_pair = stacked(grad_buf[pl.ds(first_row, BLOCK), cols])
            scores = lax.dot_general(
                key_ext[window], query_pair, contract_last, preferred_element_type=jnp.float32
            )
            dweights = lax.dot_general(
                value_ext[window], grad_pair, contract_last, preferred_element_type=jnp.float32
            )
            shift = bias[...]
            scores = scores * (score_scale * LOG2E) + jnp.concatenate([shift, shift], axis=1)
            row_max = jnp.max(scores, axis=0, keepdims=True)
            exponent = jnp.exp2(scores - row_max)
            row_total = jnp.sum(exponent, axis=0, keepdims=True)
            weights = exponent * (1.0 / row_total)
            weights_low = weights.astype(jnp.bfloat16)
            delta = jnp.sum(weights * dweights, axis=0, keepdims=True)
            dscores = (weights * (dweights - delta)).astype(jnp.bfloat16)
            key_acc[window] += jnp.dot(dscores, query_pair, preferred_element_type=jnp.float32)
            value_acc[window] += jnp.dot(weights_low, grad_pair, preferred_element_type=jnp.float32)
            totals = row_max * LN2 + jnp.log(row_total)
            for half in range(2):
                total_rows[block * pieces + piece, half : half + 1] = totals[
                    :, half * BLOCK : (half + 1) * BLOCK
                ]
            return carry

        if step == 3:
            for done in range(peers - 1):

                @pl.when((done != block) & (done != block - 1))
                def _():
                    write(done)

            @pl.when(span < spans - 1)
            def _():
                return_copy.wait_recv()
                held = pl.ds(last * BLOCK + HALO, BLOCK)
                returned = halo_recv[...].astype(jnp.float32)
                key_acc[held] += returned[:HALO]
                value_acc[held] += returned[HALO:]

            write(last)
            for done in range(peers):

                @pl.when(done != block)
                def _():
                    put_totals(done)

        lax.fori_loop(0, pieces, one_piece, 0)

        @pl.when((block == 0) & (span > 0))
        def _():
            halo_send[pl.ds(0, HALO)] = key_acc[pl.ds(0, HALO)].astype(jnp.bfloat16)
            halo_send[pl.ds(HALO, HALO)] = value_acc[pl.ds(0, HALO)].astype(jnp.bfloat16)
            return_copy.start()

    for done in range(1, peers - 1):

        @pl.when(done == final)
        def _():
            write(done - 1)
            write(done)
            put_totals(done)

    for peer in range(peers):

        @pl.when(peer != me)
        def _():
            pair_copy(0, key_buf, key_ext, me, peer).wait_send()
            pair_copy(1, value_buf, value_ext, me, peer).wait_send()
            for piece in range(pieces):
                query_copy(piece, me, peer).wait_send()

    @pl.when(span < spans - 1)
    def _():
        halo_copy(0, key_ext).wait_send()
        halo_copy(1, value_ext).wait_send()

    @pl.when(span > 0)
    def _():
        return_copy.wait_send()


def put_out(grads, totals, grads_out, totals_out, sems):
    copies = [
        pltpu.make_async_copy(grads, grads_out, sems.at[0]),
        pltpu.make_async_copy(totals, totals_out, sems.at[1]),
    ]
    for copy in copies:
        copy.start()
    for copy in copies:
        copy.wait()


def fused_shards(queries, keys, values, out_grad, doc_lengths):
    head_count = lax.axis_size("head")
    rows = queries.shape[0]
    span_len = rows * head_count
    head_cols = queries.shape[1] // head_count
    heads_here = HEADS // head_count
    pieces = heads_here // 2
    any_space = pl.BlockSpec(memory_space=pl.ANY)
    vmem = pl.BlockSpec(memory_space=pltpu.VMEM)
    dma = pltpu.SemaphoreType.DMA
    held = pl.pallas_call(
        attend_kernel,
        out_shape=(
            pltpu.VMEM((2 * HEAD_DIM, span_len), jnp.bfloat16),
            pltpu.VMEM((heads_here, span_len), jnp.float32),
        ),
        in_specs=[any_space] * 5,
        out_specs=(vmem, vmem),
        scratch_shapes=[
            pltpu.SMEM(doc_lengths.shape, jnp.int32),
            pltpu.VMEM(queries.shape, jnp.bfloat16),
            pltpu.VMEM(keys.shape, jnp.bfloat16),
            pltpu.VMEM(values.shape, jnp.bfloat16),
            pltpu.VMEM((head_count, rows, head_cols), jnp.bfloat16),
            pltpu.VMEM((HALO + span_len, HEAD_DIM), jnp.bfloat16),
            pltpu.VMEM((HALO + span_len, HEAD_DIM), jnp.bfloat16),
            pltpu.VMEM(out_grad.shape, jnp.bfloat16),
            pltpu.VMEM((WINDOW * BLOCK, BLOCK), jnp.float32),
            pltpu.VMEM((HALO + span_len, HEAD_DIM), jnp.float32),
            pltpu.VMEM((HALO + span_len, HEAD_DIM), jnp.float32),
            pltpu.VMEM((2 * HALO, HEAD_DIM), jnp.bfloat16),
            pltpu.VMEM((2 * HALO, HEAD_DIM), jnp.bfloat16),
            pltpu.VMEM((head_count * pieces, 8, BLOCK), jnp.float32),
            dma((8,)),
            dma((2, head_count)),
            dma((2, head_count)),
            dma((head_count, pieces)),
            dma((head_count, pieces)),
            dma((3,)),
            dma((3,)),
            pltpu.SemaphoreType.REGULAR((head_count,)),
            pltpu.SemaphoreType.REGULAR,
        ],
        compiler_params=pltpu.CompilerParams(collective_id=0, has_side_effects=True),
        name="attend",
    )(doc_lengths, queries, keys, values, out_grad)
    return pl.pallas_call(
        put_out,
        out_shape=tuple(jax.ShapeDtypeStruct(one.shape, one.dtype) for one in held),
        in_specs=[vmem, vmem],
        out_specs=(any_space, any_space),
        scratch_shapes=[dma((2,))],
        name="put_out",
    )(*[pltpu.with_memory_space_constraint(one, pltpu.VMEM) for one in held])


def pick_shards(queries, keys, values, out_grad, doc_lengths):
    head_count = lax.axis_size("head")
    if head_count == KV_HEADS == 4 and queries.shape[0] == BLOCK == HALO:
        return fused_shards(queries, keys, values, out_grad, doc_lengths)
    return shards(queries, keys, values, out_grad, doc_lengths)


def solution(mesh):
    return jax.shard_map(
        pick_shards,
        mesh=mesh,
        in_specs=(
            P(("rep", "span", "head"), None),
            P(("rep", "span", "head"), None),
            P(("rep", "span", "head"), None),
            P(("rep", "span"), "head"),
            P("rep"),
        ),
        out_specs=(P("head", ("rep", "span")), P("head", ("rep", "span"))),
        check_vma=False,
    )
```

```python
import math

import jax
import jax.numpy as jnp
from jax import lax
from jax.experimental import pallas as pl
from jax.experimental.pallas import tpu as pltpu
from jax.sharding import PartitionSpec as P

HEADS = 32
KV_HEADS = 4
HEAD_DIM = 128
BLOCK = 128
WINDOW = 2
HALO = 128
LOG2E = math.log2(math.e)
LN2 = math.log(2.0)
MESH = pl.DeviceIdType.MESH


def from_partner(block, axis, bit):
    count = lax.axis_size(axis)
    route = []
    for low in range(count):
        high = low | 1 << bit
        if high != low and high < count:
            route += [(low, high), (high, low)]
    return lax.ppermute(block, axis, route)


def passed_along(block, axis, distance):
    devices = range(lax.axis_size(axis))
    route = [(i - distance, i) for i in devices if i - distance in devices]
    return lax.ppermute(block, axis, route)


def group_total(partial_value, sharers, head_index):
    levels = sharers.bit_length() - 1
    for level in reversed(range(levels)):
        half_rows = partial_value.shape[0] // 2
        lower_half = head_index >> level & 1 == 0
        kept_rows = jnp.where(lower_half, partial_value[:half_rows], partial_value[half_rows:])
        given_rows = jnp.where(lower_half, partial_value[half_rows:], partial_value[:half_rows])
        partial_value = kept_rows + from_partner(given_rows, "head", level)
    return partial_value


def shards(queries, keys, values, out_grad, doc_lengths):
    head_count = lax.axis_size("head")
    head_index = lax.axis_index("head")
    span_index = lax.axis_index("span")
    tok_rows = queries.shape[0]
    heads_here = HEADS // head_count
    sharers = head_count // KV_HEADS
    span_len = tok_rows * head_count
    score_scale = 1.0 / math.sqrt(HEAD_DIM)
    query_send = queries.reshape(tok_rows, head_count, heads_here * HEAD_DIM)
    keyval = jnp.concatenate(
        [keys.reshape(tok_rows, KV_HEADS, HEAD_DIM), values.reshape(tok_rows, KV_HEADS, HEAD_DIM)],
        axis=2,
    )
    repeated = jnp.repeat(keyval, sharers, axis=1)
    query_local, pairs_local = (
        lax.all_to_all(query_send, "head", split_axis=1, concat_axis=0, tiled=True),
        lax.all_to_all(repeated, "head", split_axis=1, concat_axis=0, tiled=True),
    )
    pairs_local = pairs_local.reshape(span_len, 2 * HEAD_DIM)
    query_local = query_local.reshape(span_len, heads_here, HEAD_DIM)
    grad_local = out_grad.reshape(span_len, heads_here, HEAD_DIM)
    earlier = passed_along(pairs_local[span_len - HALO :], "span", 1)
    extended = jnp.concatenate([earlier, pairs_local], 0)
    base_row = span_index * span_len
    doc_starts = jnp.cumsum(doc_lengths) - doc_lengths
    query_pos = base_row + jnp.arange(span_len, dtype=jnp.int32)
    doc_first = jnp.max(
        jnp.where(doc_starts[None, :] <= query_pos[:, None], doc_starts[None, :], 0), axis=1
    )
    n_blocks = span_len // BLOCK
    per_group = min(n_blocks, max(1, 512 // BLOCK))
    n_groups = n_blocks // per_group
    group_rows = per_group * BLOCK
    width = WINDOW * BLOCK
    block_offsets = jnp.arange(BLOCK, dtype=jnp.int32)
    window_offsets = jnp.arange(width, dtype=jnp.int32)
    block_starts = jnp.arange(per_group, dtype=jnp.int32) * BLOCK

    def attend(gradients, group_index):
        first_row = group_index * group_rows
        query_group = lax.dynamic_slice_in_dim(query_local, first_row, group_rows, 0).reshape(
            per_group, BLOCK, heads_here, HEAD_DIM
        )
        grad_group = lax.dynamic_slice_in_dim(grad_local, first_row, group_rows, 0).reshape(
            per_group, BLOCK, heads_here, HEAD_DIM
        )
        pair_rows = lax.dynamic_slice_in_dim(extended, first_row, group_rows + HALO, 0).reshape(
            per_group + WINDOW - 1, BLOCK, 2 * HEAD_DIM
        )
        window = jnp.stack(
            [pair_rows[shift_index : shift_index + per_group] for shift_index in range(WINDOW)],
            axis=1,
        ).reshape(per_group, width, 2 * HEAD_DIM)
        key_window = window[..., :HEAD_DIM]
        value_window = window[..., HEAD_DIM:]
        query_rows = base_row + first_row + block_starts[:, None] + block_offsets[None, :]
        key_rows = base_row + first_row - HALO + block_starts[:, None] + window_offsets[None, :]
        first_doc = lax.dynamic_slice_in_dim(doc_first, first_row, group_rows, 0).reshape(
            per_group, BLOCK
        )
        allowed = (key_rows[:, None, :] >= first_doc[:, :, None]) & (
            key_rows[:, None, :] <= query_rows[:, :, None]
        )
        scores = (
            jnp.einsum(
                "gqhd,gkd->ghqk", query_group, key_window, preferred_element_type=jnp.float32
            )
            * score_scale
        )
        scores = jnp.where(allowed[:, None], scores, -1e30)
        row_max = jnp.max(scores, axis=-1, keepdims=True)
        exponent = jnp.exp(scores - row_max)
        row_total = jnp.sum(exponent, axis=-1, keepdims=True)
        weights = exponent / row_total
        log_totals = (row_max + jnp.log(row_total))[..., 0]
        weights_low = weights.astype(jnp.bfloat16)
        attention = jnp.einsum(
            "ghqk,gkd->gqhd", weights_low, value_window, preferred_element_type=jnp.float32
        ).astype(jnp.bfloat16)
        attention = lax.optimization_barrier(attention).astype(jnp.float32)
        dweights = jnp.einsum(
            "gqhd,gkd->ghqk", grad_group, value_window, preferred_element_type=jnp.float32
        )
        delta_rows = jnp.einsum("gqhd,gqhd->ghq", grad_group.astype(jnp.float32), attention)
        dscores = (weights * (dweights - delta_rows[..., None])).astype(jnp.bfloat16)
        key_part = (
            jnp.einsum("ghqk,gqhd->gkd", dscores, query_group, preferred_element_type=jnp.float32)
            * score_scale
        )
        value_part = jnp.einsum(
            "ghqk,gqhd->gkd", weights_low, grad_group, preferred_element_type=jnp.float32
        )
        pieces = jnp.concatenate([key_part, value_part], -1).reshape(
            per_group, WINDOW, BLOCK, 2 * HEAD_DIM
        )
        folded = jnp.zeros((per_group + WINDOW - 1, BLOCK, 2 * HEAD_DIM), jnp.float32)
        for shift_index in range(WINDOW):
            folded = folded.at[shift_index : shift_index + per_group].add(pieces[:, shift_index])
        folded = folded.reshape(group_rows + HALO, 2 * HEAD_DIM)
        current = lax.dynamic_slice_in_dim(gradients, first_row, group_rows + HALO, 0)
        gradients = lax.dynamic_update_slice_in_dim(gradients, current + folded, first_row, 0)
        return (gradients, jnp.transpose(log_totals, (1, 0, 2)).reshape(heads_here, group_rows))

    gradients, total_groups = lax.scan(
        attend,
        jnp.zeros((HALO + span_len, 2 * HEAD_DIM), jnp.float32),
        jnp.arange(n_groups, dtype=jnp.int32),
    )
    log_totals = jnp.transpose(total_groups, (1, 0, 2)).reshape(heads_here, span_len)
    summed = group_total(gradients.T, sharers, head_index)
    returned = passed_along(summed[:, :HALO].astype(jnp.bfloat16), "span", -1).astype(jnp.float32)
    local_grads = summed[:, HALO:].at[:, span_len - HALO :].add(returned)
    return (local_grads.astype(jnp.bfloat16), log_totals)


def attend_kernel(
    lengths_hbm, queries, keys, values, out_grad,
    grads_out, totals_out,
    lengths, query_buf, key_buf, value_buf, query_slots, key_ext, value_ext, grad_buf,
    bias, key_acc, value_acc, halo_send, halo_recv, total_rows,
    local_sems, pair_send, pair_recv, query_send, query_recv, whole_send, whole_recv, edge_send, edge_recv,
    ready, span_ready,
):
    span = lax.axis_index("span")
    spans = lax.axis_size("span")
    me = lax.axis_index("head")
    peers = lax.axis_size("head")
    last = peers - 1
    rows = queries.shape[0]
    head_cols = queries.shape[1] // peers
    piece_cols = 2 * HEAD_DIM
    pieces = head_cols // piece_cols
    width = WINDOW * BLOCK
    def by_place(*choices):
        pick = choices[0]
        for place in range(1, len(choices)):
            pick = jnp.where(me == place, choices[place], pick)
        return pick

    final = by_place(2, 2, 1, 1)
    order = (by_place(0, 1, 2, 3), by_place(3, 0, 0, 2), by_place(1, 3, 3, 0), final)

    def column(index, size):
        return pl.ds(pl.multiple_of(index * size, size), size)

    own_rows = pl.ds(pl.multiple_of(HALO + me * rows, rows), rows)
    loads = [
        pltpu.make_async_copy(keys, key_buf, local_sems.at[0]),
        pltpu.make_async_copy(values, value_buf, local_sems.at[1]),
        pltpu.make_async_copy(queries, query_buf, local_sems.at[2]),
        pltpu.make_async_copy(
            keys.at[:, column(me, HEAD_DIM)], key_ext.at[own_rows], local_sems.at[3]
        ),
        pltpu.make_async_copy(
            values.at[:, column(me, HEAD_DIM)], value_ext.at[own_rows], local_sems.at[4]
        ),
        pltpu.make_async_copy(
            queries.at[:, column(me, head_cols)], query_slots.at[me], local_sems.at[5]
        ),
        pltpu.make_async_copy(out_grad, grad_buf, local_sems.at[6]),
        pltpu.make_async_copy(lengths_hbm, lengths, local_sems.at[7]),
    ]
    for load in loads[:3]:
        load.start()

    barrier = pltpu.get_barrier_semaphore()
    for peer in range(1, peers):

        @pl.when(peer > me)
        def _():
            pl.semaphore_signal(barrier, inc=1, device_id={"head": peer}, device_id_type=MESH)

    @pl.when(span < spans - 1)
    def _():
        pl.semaphore_signal(barrier, inc=1, device_id={"span": span + 1}, device_id_type=MESH)

    @pl.when(me + span > 0)
    def _():
        pl.semaphore_wait(barrier, me + jnp.minimum(span, 1))

    for peer in range(peers - 1):

        @pl.when(peer < me)
        def _():
            pl.semaphore_signal(
                ready.at[me], inc=1, device_id={"head": peer}, device_id_type=MESH
            )

    @pl.when(span > 0)
    def _():
        pl.semaphore_signal(span_ready, inc=1, device_id={"span": span - 1}, device_id_type=MESH)

    def pair_copy(which, buf, ext, source, target):
        return pltpu.make_async_remote_copy(
            src_ref=buf.at[:, column(target, HEAD_DIM)],
            dst_ref=ext.at[pl.ds(pl.multiple_of(HALO + source * rows, rows), rows)],
            send_sem=pair_send.at[which, target],
            recv_sem=pair_recv.at[which, source],
            device_id={"head": target},
            device_id_type=MESH,
        )

    def query_copy(piece, source, target):
        return pltpu.make_async_remote_copy(
            src_ref=query_buf.at[:, column(target * pieces + piece, piece_cols)],
            dst_ref=query_slots.at[source, :, column(piece, piece_cols)],
            send_sem=query_send.at[piece],
            recv_sem=query_recv.at[piece],
            device_id={"head": target},
            device_id_type=MESH,
        )

    def send_pairs(peer):
        pair_copy(0, key_buf, key_ext, me, peer).start()
        pair_copy(1, value_buf, value_ext, me, peer).start()

    def whole_copy(source, target):
        return pltpu.make_async_remote_copy(
            src_ref=query_buf.at[:, column(target, head_cols)],
            dst_ref=query_slots.at[source],
            send_sem=whole_send.at[target],
            recv_sem=whole_recv.at[source],
            device_id={"head": target},
            device_id_type=MESH,
        )

    middle = (me > 0) & (me < last)

    def send_pieces(some):
        for piece in some:
            query_copy(piece, me, last - me).start()

    def send_up_pairs(peer):
        @pl.when(peer > me)
        def _():
            pl.semaphore_wait(ready.at[peer], 1)
            send_pairs(peer)

    def send_whole(peer, wanted):
        @pl.when(wanted)
        def _():
            whole_copy(me, peer).start()

    loads[0].wait()
    loads[1].wait()
    for peer in range(last):

        @pl.when(peer < me)
        def _():
            send_pairs(peer)

    loads[2].wait()
    send_whole(0, me > 1)
    send_whole(1, me == last)
    send_whole(2, me == last)
    send_up_pairs(1)
    send_up_pairs(2)

    @pl.when(me == 1)
    def _():
        send_pieces(range(1))

    send_up_pairs(last)
    send_whole(1, me == 0)
    send_whole(2, me == 0)
    send_whole(last, me < last)
    send_whole(0, me == 1)

    @pl.when(me == 1)
    def _():
        send_pieces(range(1, pieces))

    @pl.when(me == 2)
    def _():
        send_pieces(range(pieces))

    for load in loads[3:]:
        load.start()

    key_acc[...] = jnp.zeros_like(key_acc)
    value_acc[...] = jnp.zeros_like(value_acc)
    for load in loads[3:]:
        load.wait()

    def wait_pairs(peer, wanted=True):
        @pl.when((peer != me) & wanted)
        def _():
            pair_copy(0, key_buf, key_ext, peer, me).wait_recv()
            pair_copy(1, value_buf, value_ext, peer, me).wait_recv()

    def halo_copy(which, ext):
        return pltpu.make_async_remote_copy(
            src_ref=ext.at[pl.ds(peers * rows, HALO)],
            dst_ref=ext.at[pl.ds(0, HALO)],
            send_sem=edge_send.at[which],
            recv_sem=edge_recv.at[which],
            device_id={"span": span + 1},
            device_id_type=MESH,
        )

    return_copy = pltpu.make_async_remote_copy(
        src_ref=halo_send,
        dst_ref=halo_recv,
        send_sem=edge_send.at[2],
        recv_sem=edge_recv.at[2],
        device_id={"span": span - 1},
        device_id_type=MESH,
    )

    wait_pairs(last)

    @pl.when(span < spans - 1)
    def _():
        pl.semaphore_wait(span_ready, 1)
        halo_copy(0, key_ext).start()
        halo_copy(1, value_ext).start()


    score_scale = 1.0 / math.sqrt(HEAD_DIM)
    contract_last = (((1,), (1,)), ((), ()))

    def stacked(block):
        return jnp.concatenate([block[:, :HEAD_DIM], block[:, HEAD_DIM:]], axis=0)

    def write(done):
        held = pl.ds(HALO + done * BLOCK, BLOCK)
        cols = pl.ds(done * BLOCK, BLOCK)
        key_part = key_acc[held] * score_scale
        grads_out[pl.ds(0, HEAD_DIM), cols] = key_part.astype(jnp.bfloat16).T
        grads_out[pl.ds(HEAD_DIM, HEAD_DIM), cols] = value_acc[held].astype(jnp.bfloat16).T

    def put_totals(block):
        for head in range(2 * pieces):
            totals_out[head : head + 1, block * BLOCK : (block + 1) * BLOCK] = total_rows[
                block * pieces + head // 2, head % 2 : head % 2 + 1
            ]

    def take_return():
        @pl.when(span < spans - 1)
        def _():
            return_copy.wait_recv()
            held = pl.ds(last * BLOCK + HALO, BLOCK)
            returned = halo_recv[...].astype(jnp.float32)
            key_acc[held] += returned[:HALO]
            value_acc[held] += returned[HALO:]

        write(last)

    for step in range(4):
        block = order[step]
        for peer in range(last):
            known = False
            for before in order[:step]:
                known |= (before == peer) | (before == peer + 1)
            wait_pairs(peer, ((block == peer) | (block == peer + 1)) & jnp.logical_not(known))

        @pl.when((block == 0) & (span > 0))
        def _():
            halo_copy(0, key_ext).wait_recv()
            halo_copy(1, value_ext).wait_recv()

        @pl.when((block == 0) & (span == 0))
        def _():
            key_ext[pl.ds(0, HALO)] = jnp.zeros((HALO, HEAD_DIM), jnp.bfloat16)
            value_ext[pl.ds(0, HALO)] = jnp.zeros((HALO, HEAD_DIM), jnp.bfloat16)

        first_row = pl.multiple_of(block * BLOCK, BLOCK)
        window = pl.ds(first_row, width)
        base = (span * peers + block) * BLOCK
        query_pos = base + lax.broadcasted_iota(jnp.int32, (1, BLOCK), 1)
        first = jnp.zeros((1, BLOCK), jnp.int32)
        start = jnp.int32(0)
        for doc in range(lengths.shape[0]):
            first = jnp.maximum(first, jnp.where(query_pos >= start, start, 0))
            start = start + lengths[doc]
        key_pos = base - HALO + lax.broadcasted_iota(jnp.int32, (width, BLOCK), 0)
        allowed = (key_pos >= first) & (key_pos <= query_pos)
        bias[...] = jnp.where(allowed, 0.0, -1e30)

        def one_piece(piece, carry, block=block, first_row=first_row, window=window, step=step):
            if step == 3:

                @pl.when(middle)
                def _():
                    query_copy(piece, block, me).wait_recv()

            cols = column(piece, piece_cols)
            query_pair = stacked(query_slots[block, :, cols])
            grad_pair = stacked(grad_buf[pl.ds(first_row, BLOCK), cols])
            scores = lax.dot_general(
                key_ext[window], query_pair, contract_last, preferred_element_type=jnp.float32
            )
            dweights = lax.dot_general(
                value_ext[window], grad_pair, contract_last, preferred_element_type=jnp.float32
            )
            shift = bias[...]
            scores = scores * (score_scale * LOG2E) + jnp.concatenate([shift, shift], axis=1)
            row_max = jnp.max(scores, axis=0, keepdims=True)
            exponent = jnp.exp2(scores - row_max)
            row_total = jnp.sum(exponent, axis=0, keepdims=True)
            mixed = jnp.sum(exponent * dweights, axis=0, keepdims=True)
            inverse = 1.0 / row_total
            weights = exponent * inverse
            weights_low = weights.astype(jnp.bfloat16)
            delta = mixed * inverse
            dscores = (weights * (dweights - delta)).astype(jnp.bfloat16)
            key_acc[window] += jnp.dot(dscores, query_pair, preferred_element_type=jnp.float32)
            value_acc[window] += jnp.dot(weights_low, grad_pair, preferred_element_type=jnp.float32)
            totals = row_max * LN2 + jnp.log(row_total)
            for half in range(2):
                total_rows[block * pieces + piece, half : half + 1] = totals[
                    :, half * BLOCK : (half + 1) * BLOCK
                ]
            return carry

        if step == 3:
            for done in range(peers - 1):

                @pl.when((done != block) & (done != block - 1))
                def _():
                    write(done)

            pl.when(me < last)(take_return)
            for done in range(peers):

                @pl.when(done != block)
                def _():
                    put_totals(done)

        @pl.when((block != me) & jnp.logical_not(middle & (step == 3)))
        def _():
            whole_copy(block, me).wait_recv()

        lax.fori_loop(0, pieces, one_piece, 0)

        @pl.when((block == 0) & (span > 0))
        def _():
            halo_send[pl.ds(0, HALO)] = key_acc[pl.ds(0, HALO)].astype(jnp.bfloat16)
            halo_send[pl.ds(HALO, HALO)] = value_acc[pl.ds(0, HALO)].astype(jnp.bfloat16)
            return_copy.start()

    pl.when(me == last)(take_return)
    for done in range(1, peers - 1):

        @pl.when(done == final)
        def _():
            write(done - 1)
            write(done)
            put_totals(done)

    for peer in range(peers):

        @pl.when(peer != me)
        def _():
            pair_copy(0, key_buf, key_ext, me, peer).wait_send()
            pair_copy(1, value_buf, value_ext, me, peer).wait_send()

            @pl.when(jnp.logical_not(middle & (peer == last - me)))
            def _():
                whole_copy(me, peer).wait_send()

    @pl.when(middle)
    def _():
        for piece in range(pieces):
            query_copy(piece, me, last - me).wait_send()

    @pl.when(span < spans - 1)
    def _():
        halo_copy(0, key_ext).wait_send()
        halo_copy(1, value_ext).wait_send()

    @pl.when(span > 0)
    def _():
        return_copy.wait_send()


def put_out(grads, totals, grads_out, totals_out, sems):
    copies = [
        pltpu.make_async_copy(grads, grads_out, sems.at[0]),
        pltpu.make_async_copy(totals, totals_out, sems.at[1]),
    ]
    for copy in copies:
        copy.start()
    for copy in copies:
        copy.wait()


def fused_shards(queries, keys, values, out_grad, doc_lengths):
    head_count = lax.axis_size("head")
    rows = queries.shape[0]
    span_len = rows * head_count
    head_cols = queries.shape[1] // head_count
    heads_here = HEADS // head_count
    pieces = heads_here // 2
    any_space = pl.BlockSpec(memory_space=pl.ANY)
    vmem = pl.BlockSpec(memory_space=pltpu.VMEM)
    dma = pltpu.SemaphoreType.DMA
    held = pl.pallas_call(
        attend_kernel,
        out_shape=(
            pltpu.VMEM((2 * HEAD_DIM, span_len), jnp.bfloat16),
            pltpu.VMEM((heads_here, span_len), jnp.float32),
        ),
        in_specs=[any_space] * 5,
        out_specs=(vmem, vmem),
        scratch_shapes=[
            pltpu.SMEM(doc_lengths.shape, jnp.int32),
            pltpu.VMEM(queries.shape, jnp.bfloat16),
            pltpu.VMEM(keys.shape, jnp.bfloat16),
            pltpu.VMEM(values.shape, jnp.bfloat16),
            pltpu.VMEM((head_count, rows, head_cols), jnp.bfloat16),
            pltpu.VMEM((HALO + span_len, HEAD_DIM), jnp.bfloat16),
            pltpu.VMEM((HALO + span_len, HEAD_DIM), jnp.bfloat16),
            pltpu.VMEM(out_grad.shape, jnp.bfloat16),
            pltpu.VMEM((WINDOW * BLOCK, BLOCK), jnp.float32),
            pltpu.VMEM((HALO + span_len, HEAD_DIM), jnp.float32),
            pltpu.VMEM((HALO + span_len, HEAD_DIM), jnp.float32),
            pltpu.VMEM((2 * HALO, HEAD_DIM), jnp.bfloat16),
            pltpu.VMEM((2 * HALO, HEAD_DIM), jnp.bfloat16),
            pltpu.VMEM((head_count * pieces, 8, BLOCK), jnp.float32),
            dma((8,)),
            dma((2, head_count)),
            dma((2, head_count)),
            dma((pieces,)),
            dma((pieces,)),
            dma((head_count,)),
            dma((head_count,)),
            dma((3,)),
            dma((3,)),
            pltpu.SemaphoreType.REGULAR((head_count,)),
            pltpu.SemaphoreType.REGULAR,
        ],
        compiler_params=pltpu.CompilerParams(collective_id=0, has_side_effects=True),
        name="attend",
    )(doc_lengths, queries, keys, values, out_grad)
    return pl.pallas_call(
        put_out,
        out_shape=tuple(jax.ShapeDtypeStruct(one.shape, one.dtype) for one in held),
        in_specs=[vmem, vmem],
        out_specs=(any_space, any_space),
        scratch_shapes=[dma((2,))],
        name="put_out",
    )(*[pltpu.with_memory_space_constraint(one, pltpu.VMEM) for one in held])


def pick_shards(queries, keys, values, out_grad, doc_lengths):
    head_count = lax.axis_size("head")
    if head_count == KV_HEADS == 4 and queries.shape[0] == BLOCK == HALO:
        return fused_shards(queries, keys, values, out_grad, doc_lengths)
    return shards(queries, keys, values, out_grad, doc_lengths)


def solution(mesh):
    return jax.shard_map(
        pick_shards,
        mesh=mesh,
        in_specs=(
            P(("rep", "span", "head"), None),
            P(("rep", "span", "head"), None),
            P(("rep", "span", "head"), None),
            P(("rep", "span"), "head"),
            P("rep"),
        ),
        out_specs=(P("head", ("rep", "span")), P("head", ("rep", "span"))),
        check_vma=False,
    )
```

```python
import math

import jax
import jax.numpy as jnp
from jax import lax
from jax.experimental import pallas as pl
from jax.experimental.pallas import tpu as pltpu
from jax.sharding import PartitionSpec as P

HEADS = 32
KV_HEADS = 4
HEAD_DIM = 128
BLOCK = 128
WINDOW = 2
HALO = 128
LOG2E = math.log2(math.e)
LN2 = math.log(2.0)
MESH = pl.DeviceIdType.MESH


def from_partner(block, axis, bit):
    count = lax.axis_size(axis)
    route = []
    for low in range(count):
        high = low | 1 << bit
        if high != low and high < count:
            route += [(low, high), (high, low)]
    return lax.ppermute(block, axis, route)


def passed_along(block, axis, distance):
    devices = range(lax.axis_size(axis))
    route = [(i - distance, i) for i in devices if i - distance in devices]
    return lax.ppermute(block, axis, route)


def group_total(partial_value, sharers, head_index):
    levels = sharers.bit_length() - 1
    for level in reversed(range(levels)):
        half_rows = partial_value.shape[0] // 2
        lower_half = head_index >> level & 1 == 0
        kept_rows = jnp.where(lower_half, partial_value[:half_rows], partial_value[half_rows:])
        given_rows = jnp.where(lower_half, partial_value[half_rows:], partial_value[:half_rows])
        partial_value = kept_rows + from_partner(given_rows, "head", level)
    return partial_value


def shards(queries, keys, values, out_grad, doc_lengths):
    head_count = lax.axis_size("head")
    head_index = lax.axis_index("head")
    span_index = lax.axis_index("span")
    tok_rows = queries.shape[0]
    heads_here = HEADS // head_count
    sharers = head_count // KV_HEADS
    span_len = tok_rows * head_count
    score_scale = 1.0 / math.sqrt(HEAD_DIM)
    query_send = queries.reshape(tok_rows, head_count, heads_here * HEAD_DIM)
    keyval = jnp.concatenate(
        [keys.reshape(tok_rows, KV_HEADS, HEAD_DIM), values.reshape(tok_rows, KV_HEADS, HEAD_DIM)],
        axis=2,
    )
    repeated = jnp.repeat(keyval, sharers, axis=1)
    query_local, pairs_local = (
        lax.all_to_all(query_send, "head", split_axis=1, concat_axis=0, tiled=True),
        lax.all_to_all(repeated, "head", split_axis=1, concat_axis=0, tiled=True),
    )
    pairs_local = pairs_local.reshape(span_len, 2 * HEAD_DIM)
    query_local = query_local.reshape(span_len, heads_here, HEAD_DIM)
    grad_local = out_grad.reshape(span_len, heads_here, HEAD_DIM)
    earlier = passed_along(pairs_local[span_len - HALO :], "span", 1)
    extended = jnp.concatenate([earlier, pairs_local], 0)
    base_row = span_index * span_len
    doc_starts = jnp.cumsum(doc_lengths) - doc_lengths
    query_pos = base_row + jnp.arange(span_len, dtype=jnp.int32)
    doc_first = jnp.max(
        jnp.where(doc_starts[None, :] <= query_pos[:, None], doc_starts[None, :], 0), axis=1
    )
    n_blocks = span_len // BLOCK
    per_group = min(n_blocks, max(1, 512 // BLOCK))
    n_groups = n_blocks // per_group
    group_rows = per_group * BLOCK
    width = WINDOW * BLOCK
    block_offsets = jnp.arange(BLOCK, dtype=jnp.int32)
    window_offsets = jnp.arange(width, dtype=jnp.int32)
    block_starts = jnp.arange(per_group, dtype=jnp.int32) * BLOCK

    def attend(gradients, group_index):
        first_row = group_index * group_rows
        query_group = lax.dynamic_slice_in_dim(query_local, first_row, group_rows, 0).reshape(
            per_group, BLOCK, heads_here, HEAD_DIM
        )
        grad_group = lax.dynamic_slice_in_dim(grad_local, first_row, group_rows, 0).reshape(
            per_group, BLOCK, heads_here, HEAD_DIM
        )
        pair_rows = lax.dynamic_slice_in_dim(extended, first_row, group_rows + HALO, 0).reshape(
            per_group + WINDOW - 1, BLOCK, 2 * HEAD_DIM
        )
        window = jnp.stack(
            [pair_rows[shift_index : shift_index + per_group] for shift_index in range(WINDOW)],
            axis=1,
        ).reshape(per_group, width, 2 * HEAD_DIM)
        key_window = window[..., :HEAD_DIM]
        value_window = window[..., HEAD_DIM:]
        query_rows = base_row + first_row + block_starts[:, None] + block_offsets[None, :]
        key_rows = base_row + first_row - HALO + block_starts[:, None] + window_offsets[None, :]
        first_doc = lax.dynamic_slice_in_dim(doc_first, first_row, group_rows, 0).reshape(
            per_group, BLOCK
        )
        allowed = (key_rows[:, None, :] >= first_doc[:, :, None]) & (
            key_rows[:, None, :] <= query_rows[:, :, None]
        )
        scores = (
            jnp.einsum(
                "gqhd,gkd->ghqk", query_group, key_window, preferred_element_type=jnp.float32
            )
            * score_scale
        )
        scores = jnp.where(allowed[:, None], scores, -1e30)
        row_max = jnp.max(scores, axis=-1, keepdims=True)
        exponent = jnp.exp(scores - row_max)
        row_total = jnp.sum(exponent, axis=-1, keepdims=True)
        weights = exponent / row_total
        log_totals = (row_max + jnp.log(row_total))[..., 0]
        weights_low = weights.astype(jnp.bfloat16)
        attention = jnp.einsum(
            "ghqk,gkd->gqhd", weights_low, value_window, preferred_element_type=jnp.float32
        ).astype(jnp.bfloat16)
        attention = lax.optimization_barrier(attention).astype(jnp.float32)
        dweights = jnp.einsum(
            "gqhd,gkd->ghqk", grad_group, value_window, preferred_element_type=jnp.float32
        )
        delta_rows = jnp.einsum("gqhd,gqhd->ghq", grad_group.astype(jnp.float32), attention)
        dscores = (weights * (dweights - delta_rows[..., None])).astype(jnp.bfloat16)
        key_part = (
            jnp.einsum("ghqk,gqhd->gkd", dscores, query_group, preferred_element_type=jnp.float32)
            * score_scale
        )
        value_part = jnp.einsum(
            "ghqk,gqhd->gkd", weights_low, grad_group, preferred_element_type=jnp.float32
        )
        pieces = jnp.concatenate([key_part, value_part], -1).reshape(
            per_group, WINDOW, BLOCK, 2 * HEAD_DIM
        )
        folded = jnp.zeros((per_group + WINDOW - 1, BLOCK, 2 * HEAD_DIM), jnp.float32)
        for shift_index in range(WINDOW):
            folded = folded.at[shift_index : shift_index + per_group].add(pieces[:, shift_index])
        folded = folded.reshape(group_rows + HALO, 2 * HEAD_DIM)
        current = lax.dynamic_slice_in_dim(gradients, first_row, group_rows + HALO, 0)
        gradients = lax.dynamic_update_slice_in_dim(gradients, current + folded, first_row, 0)
        return (gradients, jnp.transpose(log_totals, (1, 0, 2)).reshape(heads_here, group_rows))

    gradients, total_groups = lax.scan(
        attend,
        jnp.zeros((HALO + span_len, 2 * HEAD_DIM), jnp.float32),
        jnp.arange(n_groups, dtype=jnp.int32),
    )
    log_totals = jnp.transpose(total_groups, (1, 0, 2)).reshape(heads_here, span_len)
    summed = group_total(gradients.T, sharers, head_index)
    returned = passed_along(summed[:, :HALO].astype(jnp.bfloat16), "span", -1).astype(jnp.float32)
    local_grads = summed[:, HALO:].at[:, span_len - HALO :].add(returned)
    return (local_grads.astype(jnp.bfloat16), log_totals)


def attend_kernel(
    lengths_hbm, queries, keys, values, out_grad,
    grads_out, totals_out,
    lengths, query_buf, pair_buf, query_slots, pair_ext, grad_buf,
    bias, key_acc, value_acc, halo_send, halo_recv, total_rows,
    local_sems, load_sems, pair_send, pair_recv, query_send, query_recv, whole_send, whole_recv, edge_send, edge_recv,
    ready, span_ready,
):
    span = lax.axis_index("span")
    spans = lax.axis_size("span")
    me = lax.axis_index("head")
    peers = lax.axis_size("head")
    last = peers - 1
    head_cols = queries.shape[1] // peers
    piece_cols = 2 * HEAD_DIM
    pieces = head_cols // piece_cols
    width = WINDOW * BLOCK
    def by_place(*choices):
        pick = choices[0]
        for place in range(1, len(choices)):
            pick = jnp.where(me == place, choices[place], pick)
        return pick

    final = by_place(2, 2, 1, 1)
    order = (by_place(0, 1, 2, 3), by_place(3, 0, 0, 2), by_place(1, 3, 3, 0), final)

    def column(index, size):
        return pl.ds(pl.multiple_of(index * size, size), size)

    def pair_load(which, operand, peer, dst):
        return pltpu.make_async_copy(
            operand.at[:, column(peer, HEAD_DIM)], dst.at[which], load_sems.at[which, peer]
        )

    def pair_loads(peer):
        return (
            pair_load(0, keys, peer, pair_buf.at[peer]),
            pair_load(1, values, peer, pair_buf.at[peer]),
        )

    def start_pair_loads(peer):
        @pl.when(peer != me)
        def _():
            for load in pair_loads(peer):
                load.start()

    for peer in range(peers):
        start_pair_loads(peer)

    query_load = pltpu.make_async_copy(queries, query_buf, local_sems.at[0])
    query_load.start()
    loads = [
        pair_load(0, keys, me, pair_ext.at[me + 1]),
        pair_load(1, values, me, pair_ext.at[me + 1]),
        pltpu.make_async_copy(
            queries.at[:, column(me, head_cols)], query_slots.at[me], local_sems.at[1]
        ),
        pltpu.make_async_copy(out_grad, grad_buf, local_sems.at[2]),
        pltpu.make_async_copy(lengths_hbm, lengths, local_sems.at[3]),
    ]

    barrier = pltpu.get_barrier_semaphore()
    for peer in range(1, peers):

        @pl.when(peer > me)
        def _():
            pl.semaphore_signal(barrier, inc=1, device_id={"head": peer}, device_id_type=MESH)

    @pl.when(span < spans - 1)
    def _():
        pl.semaphore_signal(barrier, inc=1, device_id={"span": span + 1}, device_id_type=MESH)

    @pl.when(me + span > 0)
    def _():
        pl.semaphore_wait(barrier, me + jnp.minimum(span, 1))

    for peer in range(peers - 1):

        @pl.when(peer < me)
        def _():
            pl.semaphore_signal(
                ready.at[me], inc=1, device_id={"head": peer}, device_id_type=MESH
            )

    @pl.when(span > 0)
    def _():
        pl.semaphore_signal(span_ready, inc=1, device_id={"span": span - 1}, device_id_type=MESH)

    def pair_copy(source, target):
        return pltpu.make_async_remote_copy(
            src_ref=pair_buf.at[target],
            dst_ref=pair_ext.at[source + 1],
            send_sem=pair_send.at[target],
            recv_sem=pair_recv.at[source],
            device_id={"head": target},
            device_id_type=MESH,
        )

    def query_copy(piece, source, target):
        return pltpu.make_async_remote_copy(
            src_ref=query_buf.at[:, column(target * pieces + piece, piece_cols)],
            dst_ref=query_slots.at[source, :, column(piece, piece_cols)],
            send_sem=query_send.at[piece],
            recv_sem=query_recv.at[piece],
            device_id={"head": target},
            device_id_type=MESH,
        )

    def send_pairs(peer):
        for load in pair_loads(peer):
            load.wait()
        pair_copy(me, peer).start()

    def whole_copy(source, target):
        return pltpu.make_async_remote_copy(
            src_ref=query_buf.at[:, column(target, head_cols)],
            dst_ref=query_slots.at[source],
            send_sem=whole_send.at[target],
            recv_sem=whole_recv.at[source],
            device_id={"head": target},
            device_id_type=MESH,
        )

    middle = (me > 0) & (me < last)

    def send_pieces(some):
        for piece in some:
            query_copy(piece, me, last - me).start()

    def send_up_pairs(peer):
        @pl.when(peer > me)
        def _():
            pl.semaphore_wait(ready.at[peer], 1)
            send_pairs(peer)

    def send_whole(peer, wanted):
        @pl.when(wanted)
        def _():
            whole_copy(me, peer).start()

    for peer in range(last):

        @pl.when(peer < me)
        def _():
            send_pairs(peer)

    query_load.wait()
    send_whole(0, me > 1)
    send_whole(1, me == last)
    send_whole(2, me == last)
    send_up_pairs(1)
    send_up_pairs(2)

    @pl.when(me == 1)
    def _():
        send_pieces(range(1))

    send_up_pairs(last)
    send_whole(1, me == 0)
    send_whole(2, me == 0)
    send_whole(last, me < last)
    send_whole(0, me == 1)

    @pl.when(me == 1)
    def _():
        send_pieces(range(1, pieces))

    @pl.when(me == 2)
    def _():
        send_pieces(range(pieces))

    for load in loads:
        load.start()

    key_acc[...] = jnp.zeros_like(key_acc)
    value_acc[...] = jnp.zeros_like(value_acc)
    for load in loads:
        load.wait()

    def wait_pairs(peer, wanted=True):
        @pl.when((peer != me) & wanted)
        def _():
            pair_copy(peer, me).wait_recv()

    halo_copy = pltpu.make_async_remote_copy(
        src_ref=pair_ext.at[peers],
        dst_ref=pair_ext.at[0],
        send_sem=edge_send.at[0],
        recv_sem=edge_recv.at[0],
        device_id={"span": span + 1},
        device_id_type=MESH,
    )

    return_copy = pltpu.make_async_remote_copy(
        src_ref=halo_send,
        dst_ref=halo_recv,
        send_sem=edge_send.at[1],
        recv_sem=edge_recv.at[1],
        device_id={"span": span - 1},
        device_id_type=MESH,
    )

    wait_pairs(last)

    @pl.when(span < spans - 1)
    def _():
        pl.semaphore_wait(span_ready, 1)
        halo_copy.start()


    score_scale = 1.0 / math.sqrt(HEAD_DIM)
    contract_last = (((1,), (1,)), ((), ()))

    def stacked(block):
        return jnp.concatenate([block[:, :HEAD_DIM], block[:, HEAD_DIM:]], axis=0)

    def write(done):
        held = pl.ds(HALO + done * BLOCK, BLOCK)
        cols = pl.ds(done * BLOCK, BLOCK)
        key_part = key_acc[held] * score_scale
        grads_out[pl.ds(0, HEAD_DIM), cols] = key_part.astype(jnp.bfloat16).T
        grads_out[pl.ds(HEAD_DIM, HEAD_DIM), cols] = value_acc[held].astype(jnp.bfloat16).T

    def put_totals(block):
        for head in range(2 * pieces):
            totals_out[head : head + 1, block * BLOCK : (block + 1) * BLOCK] = total_rows[
                block * pieces + head // 2, head % 2 : head % 2 + 1
            ]

    def take_return():
        @pl.when(span < spans - 1)
        def _():
            return_copy.wait_recv()
            held = pl.ds(last * BLOCK + HALO, BLOCK)
            returned = halo_recv[...].astype(jnp.float32)
            key_acc[held] += returned[:HALO]
            value_acc[held] += returned[HALO:]

        write(last)

    for step in range(4):
        block = order[step]
        for peer in range(last):
            known = False
            for before in order[:step]:
                known |= (before == peer) | (before == peer + 1)
            wait_pairs(peer, ((block == peer) | (block == peer + 1)) & jnp.logical_not(known))

        @pl.when((block == 0) & (span > 0))
        def _():
            halo_copy.wait_recv()

        @pl.when((block == 0) & (span == 0))
        def _():
            pair_ext[0] = jnp.zeros((2, HALO, HEAD_DIM), jnp.bfloat16)

        first_row = pl.multiple_of(block * BLOCK, BLOCK)
        window = pl.ds(first_row, width)
        base = (span * peers + block) * BLOCK
        query_pos = base + lax.broadcasted_iota(jnp.int32, (1, BLOCK), 1)
        first = jnp.zeros((1, BLOCK), jnp.int32)
        start = jnp.int32(0)
        for doc in range(lengths.shape[0]):
            first = jnp.maximum(first, jnp.where(query_pos >= start, start, 0))
            start = start + lengths[doc]
        key_pos = base - HALO + lax.broadcasted_iota(jnp.int32, (width, BLOCK), 0)
        allowed = (key_pos >= first) & (key_pos <= query_pos)
        bias[...] = jnp.where(allowed, 0.0, -1e30)

        def one_piece(piece, carry, block=block, first_row=first_row, window=window, step=step):
            if step == 3:

                @pl.when(middle)
                def _():
                    query_copy(piece, block, me).wait_recv()

            def windowed(which):
                return jnp.concatenate([pair_ext[block, which], pair_ext[block + 1, which]], axis=0)

            cols = column(piece, piece_cols)
            query_pair = stacked(query_slots[block, :, cols])
            grad_pair = stacked(grad_buf[pl.ds(first_row, BLOCK), cols])
            scores = lax.dot_general(
                windowed(0), query_pair, contract_last, preferred_element_type=jnp.float32
            )
            dweights = lax.dot_general(
                windowed(1), grad_pair, contract_last, preferred_element_type=jnp.float32
            )
            shift = bias[...]
            scores = scores * (score_scale * LOG2E) + jnp.concatenate([shift, shift], axis=1)
            row_max = jnp.max(scores, axis=0, keepdims=True)
            exponent = jnp.exp2(scores - row_max)
            row_total = jnp.sum(exponent, axis=0, keepdims=True)
            mixed = jnp.sum(exponent * dweights, axis=0, keepdims=True)
            inverse = 1.0 / row_total
            weights = exponent * inverse
            weights_low = weights.astype(jnp.bfloat16)
            delta = mixed * inverse
            dscores = (weights * (dweights - delta)).astype(jnp.bfloat16)
            key_acc[window] += jnp.dot(dscores, query_pair, preferred_element_type=jnp.float32)
            value_acc[window] += jnp.dot(weights_low, grad_pair, preferred_element_type=jnp.float32)
            totals = row_max * LN2 + jnp.log(row_total)
            for half in range(2):
                total_rows[block * pieces + piece, half : half + 1] = totals[
                    :, half * BLOCK : (half + 1) * BLOCK
                ]
            return carry

        if step == 3:
            for done in range(peers - 1):

                @pl.when((done != block) & (done != block - 1))
                def _():
                    write(done)

            pl.when(me < last)(take_return)
            for done in range(peers):

                @pl.when(done != block)
                def _():
                    put_totals(done)

        @pl.when((block != me) & jnp.logical_not(middle & (step == 3)))
        def _():
            whole_copy(block, me).wait_recv()

        lax.fori_loop(0, pieces, one_piece, 0)

        @pl.when((block == 0) & (span > 0))
        def _():
            halo_send[pl.ds(0, HALO)] = key_acc[pl.ds(0, HALO)].astype(jnp.bfloat16)
            halo_send[pl.ds(HALO, HALO)] = value_acc[pl.ds(0, HALO)].astype(jnp.bfloat16)
            return_copy.start()

    pl.when(me == last)(take_return)
    for done in range(1, peers - 1):

        @pl.when(done == final)
        def _():
            write(done - 1)
            write(done)
            put_totals(done)

    for peer in range(peers):

        @pl.when(peer != me)
        def _():
            pair_copy(me, peer).wait_send()

            @pl.when(jnp.logical_not(middle & (peer == last - me)))
            def _():
                whole_copy(me, peer).wait_send()

    @pl.when(middle)
    def _():
        for piece in range(pieces):
            query_copy(piece, me, last - me).wait_send()

    @pl.when(span < spans - 1)
    def _():
        halo_copy.wait_send()

    @pl.when(span > 0)
    def _():
        return_copy.wait_send()


def put_out(grads, totals, grads_out, totals_out, sems):
    copies = [
        pltpu.make_async_copy(grads, grads_out, sems.at[0]),
        pltpu.make_async_copy(totals, totals_out, sems.at[1]),
    ]
    for copy in copies:
        copy.start()
    for copy in copies:
        copy.wait()


def fused_shards(queries, keys, values, out_grad, doc_lengths):
    head_count = lax.axis_size("head")
    rows = queries.shape[0]
    span_len = rows * head_count
    head_cols = queries.shape[1] // head_count
    heads_here = HEADS // head_count
    pieces = heads_here // 2
    any_space = pl.BlockSpec(memory_space=pl.ANY)
    vmem = pl.BlockSpec(memory_space=pltpu.VMEM)
    dma = pltpu.SemaphoreType.DMA
    held = pl.pallas_call(
        attend_kernel,
        out_shape=(
            pltpu.VMEM((2 * HEAD_DIM, span_len), jnp.bfloat16),
            pltpu.VMEM((heads_here, span_len), jnp.float32),
        ),
        in_specs=[any_space] * 5,
        out_specs=(vmem, vmem),
        scratch_shapes=[
            pltpu.SMEM(doc_lengths.shape, jnp.int32),
            pltpu.VMEM(queries.shape, jnp.bfloat16),
            pltpu.VMEM((head_count, 2, rows, HEAD_DIM), jnp.bfloat16),
            pltpu.VMEM((head_count, rows, head_cols), jnp.bfloat16),
            pltpu.VMEM((1 + head_count, 2, rows, HEAD_DIM), jnp.bfloat16),
            pltpu.VMEM(out_grad.shape, jnp.bfloat16),
            pltpu.VMEM((WINDOW * BLOCK, BLOCK), jnp.float32),
            pltpu.VMEM((HALO + span_len, HEAD_DIM), jnp.float32),
            pltpu.VMEM((HALO + span_len, HEAD_DIM), jnp.float32),
            pltpu.VMEM((2 * HALO, HEAD_DIM), jnp.bfloat16),
            pltpu.VMEM((2 * HALO, HEAD_DIM), jnp.bfloat16),
            pltpu.VMEM((head_count * pieces, 8, BLOCK), jnp.float32),
            dma((4,)),
            dma((2, head_count)),
            dma((head_count,)),
            dma((head_count,)),
            dma((pieces,)),
            dma((pieces,)),
            dma((head_count,)),
            dma((head_count,)),
            dma((2,)),
            dma((2,)),
            pltpu.SemaphoreType.REGULAR((head_count,)),
            pltpu.SemaphoreType.REGULAR,
        ],
        compiler_params=pltpu.CompilerParams(collective_id=0, has_side_effects=True),
        name="attend",
    )(doc_lengths, queries, keys, values, out_grad)
    return pl.pallas_call(
        put_out,
        out_shape=tuple(jax.ShapeDtypeStruct(one.shape, one.dtype) for one in held),
        in_specs=[vmem, vmem],
        out_specs=(any_space, any_space),
        scratch_shapes=[dma((2,))],
        name="put_out",
    )(*[pltpu.with_memory_space_constraint(one, pltpu.VMEM) for one in held])


def pick_shards(queries, keys, values, out_grad, doc_lengths):
    head_count = lax.axis_size("head")
    if head_count == KV_HEADS == 4 and queries.shape[0] == BLOCK == HALO:
        return fused_shards(queries, keys, values, out_grad, doc_lengths)
    return shards(queries, keys, values, out_grad, doc_lengths)


def solution(mesh):
    return jax.shard_map(
        pick_shards,
        mesh=mesh,
        in_specs=(
            P(("rep", "span", "head"), None),
            P(("rep", "span", "head"), None),
            P(("rep", "span", "head"), None),
            P(("rep", "span"), "head"),
            P("rep"),
        ),
        out_specs=(P("head", ("rep", "span")), P("head", ("rep", "span"))),
        check_vma=False,
    )
```
